512 devices in a mesh: member: 16 (over x, y_hi, core), tile: 32 (over y_lo, z).
Axes of the slice: x: 4, y: 8 (y_hi: 2, y_lo: 4; y = y_hi * 4 + y_lo), z: 8, core: 2. Of those that a mesh axis runs over, the one named last changes fastest.
Arguments:
- states: bfloat16 [16, 8, 2048, 2048], P('member', None, 'tile'), may hold values from -8 to 8
- obs_var: float32 [8], replicated, may hold values from 2 to 30
- relax_rate: float32 [8], replicated, may hold values from 0.3 to 1
Outputs:
- nudged: bfloat16 [16, 8, 2048, 2048], P('member', None, 'tile')
- spread: float32 [8, 256, 256], P(None, 'tile')
The draws below stay inside these ranges and needn't reach their ends.
All inputs are finite; a program needn't handle non-finite values.
Results may differ from the reference program's by a relative error of at most 0.0034.
Values may be sent and summed in bfloat16 or wider, within the bound.
No kernel may reach another device: no remote copies, remote signals or barrier semaphores. Data moves between devices by JAX's collectives and lax.ppermute only.
A program may use at most 64 MiB of HBM per device.

```python
import math
import jax
import jax.numpy as jnp
from jax import lax

NX = 2048
NY = 2048
MODES = 256
LEVELS = 8
MEMBERS = 16


def draw_table(extent, mode_count):
    positions = jnp.arange(extent, dtype=jnp.int32)
    mode_index = jnp.arange(mode_count, dtype=jnp.int32)[None, :]
    wavenum = (mode_index + 1) // 2
    phases = positions[:, None] * wavenum % extent
    angles = 2.0 * math.pi / extent * phases.astype(jnp.float32)
    scaled = jnp.where(mode_index % 2 == 1, jnp.sin(angles), jnp.cos(angles))
    factor = jnp.where(mode_index == 0, math.sqrt(1.0 / extent), math.sqrt(2.0 / extent))
    return (scaled * factor).astype(jnp.float32)


def draw_states(key, part):
    key_noise, key_modes = jax.random.split(jax.random.fold_in(key, 11), 2)
    table_x = draw_table(NX, MODES)
    table_y = draw_table(NY, MODES)
    noise = 0.5 * jax.random.normal(key_noise, (MEMBERS, LEVELS, NX, NY), jnp.float32)
    modal = 4.0 * jax.random.normal(key_modes, (MEMBERS, LEVELS, MODES, MODES), jnp.float32)

    def expand(member_modes):
        half = jnp.einsum('ia,lab->lib', table_x, member_modes, precision=lax.Precision.HIGHEST)
        return jnp.einsum('lib,jb->lij', half, table_y, precision=lax.Precision.HIGHEST)
    smooth = lax.map(expand, modal)
    return jnp.clip(noise + smooth, -8.0, 8.0).astype(jnp.bfloat16)


def setup_inputs(seed: int = 0) -> dict:
    splits = jax.random.split(jax.random.key(seed), 4)
    states = draw_states(jax.random.fold_in(splits[3], 71), 0)
    obs_var = jnp.clip(jnp.exp(jax.random.uniform(splits[1], (LEVELS,), jnp.float32, math.log(2.0), math.log(30.0))), 2.0, 30.0)
    relax_rate = jnp.clip(jax.random.uniform(splits[2], (LEVELS,), jnp.float32, 0.3, 1.0), 0.3, 1.0)
    return {"states": states, "obs_var": obs_var, "relax_rate": relax_rate}


def mode_table(positions, extent, mode_count):
    mode_index = jnp.arange(mode_count, dtype=jnp.int32)[None, :]
    wavenum = (mode_index + 1) // 2
    phases = positions[:, None] * wavenum % extent
    angles = 2.0 * math.pi / extent * phases.astype(jnp.float32)
    scaled = jnp.where(mode_index % 2 == 1, jnp.sin(angles), jnp.cos(angles))
    factor = jnp.where(mode_index == 0, math.sqrt(1.0 / extent), math.sqrt(2.0 / extent))
    return (scaled * factor).astype(jnp.float32)

def reference(states, obs_var, relax_rate):
    levels = states.shape[1]
    table_x = mode_table(jnp.arange(NX, dtype=jnp.int32), NX, MODES)
    table_y = mode_table(jnp.arange(NY, dtype=jnp.int32), NY, MODES)
    by_half = table_y.astype(jnp.bfloat16)

    def project(member_field):
        projected = jnp.dot(member_field.reshape(levels * NX, NY), by_half, preferred_element_type=jnp.float32)
        projected = projected.reshape(levels, NX, MODES)
        return jnp.einsum('ia,lib->lab', table_x, projected, precision=lax.Precision.HIGHEST)
    coeffs = lax.map(project, states)
    departure = coeffs - coeffs[0][None]
    totals = lax.optimization_barrier(jnp.sum(departure, axis=0))
    squares = lax.optimization_barrier(jnp.sum(departure * departure, axis=0))
    mean_departure = totals / MEMBERS
    spread = squares / MEMBERS - mean_departure * mean_departure
    weight_gain = relax_rate[:, None, None] * spread / (spread + obs_var[:, None, None])

    def nudge(pair):
        member_field, member_departure = pair
        misfit = -weight_gain * member_departure
        rows_back = jnp.einsum('ia,lab->lib', table_x, misfit, precision=lax.Precision.HIGHEST).astype(jnp.bfloat16)
        increment = jnp.dot(rows_back.reshape(levels * NX, MODES), by_half.T, preferred_element_type=jnp.float32)
        increment = increment.reshape(levels, NX, NY)
        return (member_field.astype(jnp.float32) + increment).astype(jnp.bfloat16)
    nudged = lax.map(nudge, (states, departure))
    return (nudged, spread)
```

```python
import functools
import math

import jax
import jax.numpy as jnp
import numpy as np
from jax import lax
from jax.experimental import pallas as pl
from jax.experimental.pallas import tpu as pltpu
from jax.sharding import Mesh, PartitionSpec as P

N = 2048
MODES = 256
LEVELS = 8
MEMBERS = 16
TILES = 32
ROWS = N // TILES
NEAR = 4
FAR = MEMBERS // NEAR
OWN = MODES // TILES
BF16 = jnp.bfloat16
F32 = jnp.float32


def mode_table():
    mode = np.arange(MODES)[None, :]
    phases = (np.arange(N)[:, None] * ((mode + 1) // 2)) % N
    angles = 2.0 * math.pi / N * phases
    scaled = np.where(mode % 2 == 1, np.sin(angles), np.cos(angles))
    factor = np.where(mode == 0, math.sqrt(1.0 / N), math.sqrt(2.0 / N))
    return (scaled * factor).astype(np.float32)


def tables():
    full = mode_table()
    half = full.astype(BF16)
    first = np.arange(MODES).reshape(TILES, OWN).T.reshape(-1)
    second = np.arange(MODES).reshape(OWN, TILES).T.reshape(-1)
    bx = full[:, first]
    bx_high = bx.astype(BF16)
    bx_low = (bx - bx_high.astype(np.float32)).astype(BF16)
    by = half[:, second]
    return bx_high, bx_low, by, np.ascontiguousarray(by.T)


def dot(a, b, dims):
    return lax.dot_general(a, b, (dims, ((), ())), preferred_element_type=F32)


def project_kernel(states_ref, by_ref, out_ref):
    field = states_ref[...].reshape(2 * ROWS, N)
    half = dot(field, by_ref[...], ((1,), (0,)))
    out_ref[...] = half.T.reshape(TILES, 1, OWN, 2 * ROWS).astype(BF16)


def coeffs_kernel(rows_ref, high_ref, low_ref, out_ref, copies_ref, wide):
    for u in range(TILES // 2):
        a, b = rows_ref[2 * u], rows_ref[2 * u + 1]
        cols = pl.ds(2 * ROWS * u, 2 * ROWS)
        wide[: NEAR * OWN, cols] = jnp.concatenate([a[:, :ROWS], b[:, :ROWS]], axis=1)
        wide[NEAR * OWN :, cols] = jnp.concatenate([a[:, ROWS:], b[:, ROWS:]], axis=1)
    x = wide[...]
    coeffs = dot(x, high_ref[...], ((1,), (0,))) + dot(x, low_ref[...], ((1,), (0,)))
    out_ref[...] = coeffs
    for k in range(FAR):
        copies_ref[k] = coeffs


def nudge_kernel(all_ref, own_ref, obs_ref, relax_ref, high_ref, low_ref, rows_ref, spread_ref):
    pair = lax.axis_index("near")
    spreads, misfits = [], []
    for l in range(2):
        def block(ref, k):
            return ref[pl.ds(NEAR * OWN * l + OWN * k, OWN), :]

        driver = block(all_ref.at[0], 0)
        departures = [
            block(all_ref.at[f], k) - driver for f in range(FAR) for k in range(NEAR)
        ]
        mean = sum(departures[1:], departures[0]) * (1.0 / MEMBERS)
        centered = [d - mean for d in departures]
        squares = [c * c for c in centered]
        spread = sum(squares[1:], squares[0]) * (1.0 / MEMBERS)
        gain = relax_ref[2 * pair + l] * spread / (spread + obs_ref[2 * pair + l])
        spreads.append(spread)
        misfits.extend([-gain * (block(own_ref, k) - driver) for k in range(NEAR)])
    misfit = jnp.concatenate(misfits, axis=0)
    high = misfit.astype(BF16)
    low = (misfit - high.astype(F32)).astype(BF16)
    nt = ((1,), (1,))
    back = dot(high, high_ref[...], nt) + dot(low, high_ref[...], nt) + dot(high, low_ref[...], nt)
    back = back.astype(BF16)
    for u in range(TILES // 2):
        a = back[: NEAR * OWN, 2 * ROWS * u : 2 * ROWS * (u + 1)]
        b = back[NEAR * OWN :, 2 * ROWS * u : 2 * ROWS * (u + 1)]
        rows_ref[2 * u] = jnp.concatenate([a[:, :ROWS], b[:, :ROWS]], axis=1)
        rows_ref[2 * u + 1] = jnp.concatenate([a[:, ROWS:], b[:, ROWS:]], axis=1)
    both = jnp.concatenate(spreads, axis=0)
    stacked = jnp.concatenate([both[:, TILES * k : TILES * (k + 1)] for k in range(OWN)], axis=0)
    flipped = stacked.T
    high = flipped.astype(BF16)
    spread_ref[0] = high
    spread_ref[1] = (flipped - high.astype(F32)).astype(BF16)


def apply_kernel(states_ref, back_ref, parts_ref, by_ref, out_ref, spread_ref, mixed, turned):
    modes = back_ref[...].reshape(MODES, 2 * ROWS)
    increment = dot(modes, by_ref[...], ((0,), (0,)))
    field = states_ref[...].reshape(2 * ROWS, N)
    out_ref[...] = (field.astype(F32) + increment).astype(BF16).reshape(2, ROWS, N)

    @pl.when(pl.program_id(0) == 0)
    def _():
        mixed[...] = parts_ref[0].astype(F32) + parts_ref[1].astype(F32)
        ordered = jnp.concatenate(
            [mixed[pl.ds(c, TILES, stride=NEAR), :] for c in range(NEAR)], axis=0
        )
        turned[...] = ordered.T
        for l in range(2):
            strips = [turned[pl.ds(OWN * l + k, OWN, stride=2 * OWN), :] for k in range(OWN)]
            for c in range(NEAR):
                spread_ref[2 * c + l] = jnp.concatenate(
                    [s[:, TILES * c : TILES * (c + 1)] for s in strips], axis=1
                )


def call(kernel, outs, **kw):
    return pl.pallas_call(
        kernel,
        out_shape=outs,
        compiler_params=pltpu.CompilerParams(vmem_limit_bytes=24 * 1024 * 1024),
        **kw,
    )


def shape(dims, dtype):
    return jax.ShapeDtypeStruct(dims, dtype)


def per_device(consts, states, obs_var, relax_rate):
    bx_high, bx_low, by, by_t = consts
    field = states[0]
    whole = lambda *dims: pl.BlockSpec(dims, lambda i: (0,) * len(dims))
    levels = pl.BlockSpec((2, ROWS, N), lambda i: (i, 0, 0))
    chunks = pl.BlockSpec((TILES, 1, OWN, 2 * ROWS), lambda i: (0, i, 0, 0))
    smem = pl.BlockSpec(memory_space=pltpu.SMEM)
    vmem = pl.BlockSpec(memory_space=pltpu.VMEM)

    sent = call(
        project_kernel,
        shape((TILES, NEAR, OWN, 2 * ROWS), BF16),
        grid=(NEAR,),
        in_specs=[levels, whole(N, MODES)],
        out_specs=chunks,
    )(field, by)
    rows = lax.all_to_all(
        sent.reshape(TILES * NEAR, OWN, 2 * ROWS), ("tile", "near"), 0, 0, tiled=True
    )
    coeffs, copies = call(
        coeffs_kernel,
        (shape((2 * NEAR * OWN, MODES), F32), shape((FAR, 2 * NEAR * OWN, MODES), F32)),
        in_specs=[vmem] * 3,
        out_specs=(vmem, vmem),
        scratch_shapes=[pltpu.VMEM((2 * NEAR * OWN, N), BF16)],
    )(rows.reshape(TILES, NEAR * OWN, 2 * ROWS), bx_high, bx_low)
    gathered = lax.all_to_all(copies, "far", 0, 0, tiled=True)
    back, parts = call(
        nudge_kernel,
        (shape((TILES, NEAR * OWN, 2 * ROWS), BF16), shape((2, TILES, 2 * OWN * OWN), BF16)),
        in_specs=[vmem, vmem, smem, smem, vmem, vmem],
        out_specs=(vmem, vmem),
    )(gathered, coeffs, obs_var, relax_rate, bx_high, bx_low)
    extra = jnp.broadcast_to(
        jnp.transpose(parts, (1, 0, 2))[:, None, None], (TILES, NEAR, 1, 2, 2 * ROWS)
    )
    out = jnp.concatenate([back.reshape(TILES, NEAR, 4, 2, 2 * ROWS), extra], axis=2)
    got = lax.all_to_all(
        out.reshape(TILES * NEAR, 5, 2, 2 * ROWS), ("tile", "near"), 0, 0, tiled=True
    )
    modes = got[:, :4].reshape(TILES, NEAR, OWN, 2 * ROWS)
    parts = jnp.transpose(got[:, 4], (1, 0, 2))
    nudged, spread = call(
        apply_kernel,
        (shape((LEVELS, ROWS, N), BF16), shape((LEVELS, OWN, MODES), F32)),
        grid=(NEAR,),
        in_specs=[levels, chunks, whole(2, TILES * NEAR, 2 * ROWS), whole(MODES, N)],
        out_specs=(levels, whole(LEVELS, OWN, MODES)),
        scratch_shapes=[pltpu.VMEM((2 * ROWS, 2 * ROWS), F32)] * 2,
    )(field, modes, parts, by_t)
    return nudged[None], spread


def solution(mesh):
    fine = Mesh(mesh.devices.reshape(FAR, NEAR, TILES), ("far", "near", "tile"))
    rows = P(("far", "near"), None, "tile", None)
    return jax.shard_map(
        functools.partial(per_device, tables()),
        mesh=fine,
        in_specs=(rows, P(), P()),
        out_specs=(rows, P(None, "tile", None)),
        check_vma=False,
    )
```

```python
import functools
import math

import jax
import jax.numpy as jnp
import numpy as np
from jax import lax
from jax.experimental import pallas as pl
from jax.experimental.pallas import tpu as pltpu
from jax.sharding import Mesh, PartitionSpec as P

N = 2048
MODES = 256
LEVELS = 8
MEMBERS = 16
TILES = 32
ROWS = N // TILES
NEAR = 4
FAR = MEMBERS // NEAR
OWN = MODES // TILES
STEPS = 4
MIB = 1024 * 1024
BF16 = jnp.bfloat16
F32 = jnp.float32


def mode_table():
    mode = np.arange(MODES)[None, :]
    phases = (np.arange(N)[:, None] * ((mode + 1) // 2)) % N
    angles = 2.0 * math.pi / N * phases
    scaled = np.where(mode % 2 == 1, np.sin(angles), np.cos(angles))
    factor = np.where(mode == 0, math.sqrt(1.0 / N), math.sqrt(2.0 / N))
    return (scaled * factor).astype(np.float32)


def tables():
    full = mode_table()
    half = full.astype(BF16)
    first = np.arange(MODES).reshape(TILES, OWN).T.reshape(-1)
    second = np.arange(MODES).reshape(OWN, TILES).T.reshape(-1)
    bx = full[:, first]
    bx_high = bx.astype(BF16)
    bx_low = (bx - bx_high.astype(np.float32)).astype(BF16)
    by = half[:, second]
    flip = lambda a: np.ascontiguousarray(a.T)
    return bx_high, bx_low, flip(bx_high), flip(bx_low), by, flip(by)


def dot(a, b, dims):
    return lax.dot_general(a, b, (dims, ((), ())), preferred_element_type=F32)


def project_kernel(states_ref, by_ref, out_ref, field, table, acc, sems):
    width = N // STEPS

    def copies(k):
        cols = pl.ds(width * k, width)
        return (
            pltpu.make_async_copy(by_ref.at[cols, :], table.at[k], sems.at[2 * k]),
            pltpu.make_async_copy(states_ref.at[:, :, cols], field.at[k], sems.at[2 * k + 1]),
        )

    for k in range(STEPS):
        for c in copies(k):
            c.start()
    for k in range(STEPS):
        for c in copies(k):
            c.wait()
        part = dot(field[k].reshape(LEVELS * ROWS, width), table[k], ((1,), (0,)))
        acc[...] = part if k == 0 else acc[...] + part
    for c in range(NEAR):
        half = acc[2 * ROWS * c : 2 * ROWS * (c + 1), :]
        out_ref[:, c] = half.astype(BF16).T.reshape(TILES, OWN, 2 * ROWS)


def coeffs_kernel(rows_ref, high_ref, low_ref, out_ref, copies_ref, wide):
    for u in range(TILES // 2):
        a, b = rows_ref[2 * u], rows_ref[2 * u + 1]
        cols = pl.ds(2 * ROWS * u, 2 * ROWS)
        wide[: NEAR * OWN, cols] = jnp.concatenate([a[:, :ROWS], b[:, :ROWS]], axis=1)
        wide[NEAR * OWN :, cols] = jnp.concatenate([a[:, ROWS:], b[:, ROWS:]], axis=1)
    x = wide[...]
    coeffs = dot(x, high_ref[...], ((1,), (0,))) + dot(x, low_ref[...], ((1,), (0,)))
    out_ref[...] = coeffs
    for k in range(FAR):
        copies_ref[k] = coeffs


def nudge_kernel(all_ref, own_ref, obs_ref, relax_ref, high_ref, low_ref, rows_ref, spread_ref):
    pair = lax.axis_index("near")
    spreads, misfits = [], []
    for l in range(2):
        def block(ref, k):
            return ref[pl.ds(NEAR * OWN * l + OWN * k, OWN), :]

        driver = block(all_ref.at[0], 0)
        departures = [
            block(all_ref.at[f], k) - driver for f in range(FAR) for k in range(NEAR)
        ]
        mean = sum(departures[1:], departures[0]) * (1.0 / MEMBERS)
        centered = [d - mean for d in departures]
        squares = [c * c for c in centered]
        spread = sum(squares[1:], squares[0]) * (1.0 / MEMBERS)
        gain = relax_ref[2 * pair + l] * spread / (spread + obs_ref[2 * pair + l])
        spreads.append(spread)
        misfits.extend([-gain * (block(own_ref, k) - driver) for k in range(NEAR)])
    misfit = jnp.concatenate(misfits, axis=0)
    high = misfit.astype(BF16)
    low = (misfit - high.astype(F32)).astype(BF16)
    nn = ((1,), (0,))
    count = 2 * NEAR * OWN
    both = dot(jnp.concatenate([high, low], axis=0), high_ref[...], nn)
    back = both[:count] + both[count:] + dot(high, low_ref[...], nn)
    back = back.astype(BF16)
    for u in range(TILES // 2):
        a = back[: NEAR * OWN, 2 * ROWS * u : 2 * ROWS * (u + 1)]
        b = back[NEAR * OWN :, 2 * ROWS * u : 2 * ROWS * (u + 1)]
        rows_ref[2 * u] = jnp.concatenate([a[:, :ROWS], b[:, :ROWS]], axis=1)
        rows_ref[2 * u + 1] = jnp.concatenate([a[:, ROWS:], b[:, ROWS:]], axis=1)
    both = jnp.concatenate(spreads, axis=0)
    stacked = jnp.concatenate([both[:, TILES * k : TILES * (k + 1)] for k in range(OWN)], axis=0)
    flipped = stacked.T
    high = flipped.astype(BF16)
    spread_ref[0] = high
    spread_ref[1] = (flipped - high.astype(F32)).astype(BF16)


def apply_kernel(
    states_ref, back_ref, parts_ref, by_ref, out_ref, spread_ref, modes, filled, mixed, turned, sems
):
    width = N // STEPS
    for c in range(NEAR):
        block = back_ref[:, c].reshape(MODES, 2 * ROWS)
        modes[2 * ROWS * c : 2 * ROWS * (c + 1), :] = block.T

    def copy(k):
        cols = pl.ds(width * k, width)
        return pltpu.make_async_copy(filled.at[k], out_ref.at[:, :, cols], sems.at[k])

    for k in range(STEPS):
        cols = slice(width * k, width * (k + 1))
        increment = dot(modes[...], by_ref[:, cols], ((1,), (0,)))
        field = states_ref[:, :, cols].astype(F32)
        filled[k] = (field + increment.reshape(LEVELS, ROWS, width)).astype(BF16)
        copy(k).start()

    mixed[...] = parts_ref[0].astype(F32) + parts_ref[1].astype(F32)
    ordered = jnp.concatenate(
        [mixed[pl.ds(c, TILES, stride=NEAR), :] for c in range(NEAR)], axis=0
    )
    turned[...] = ordered.T
    for l in range(2):
        strips = [turned[pl.ds(OWN * l + k, OWN, stride=2 * OWN), :] for k in range(OWN)]
        for c in range(NEAR):
            spread_ref[2 * c + l] = jnp.concatenate(
                [s[:, TILES * c : TILES * (c + 1)] for s in strips], axis=1
            )
    for k in range(STEPS):
        copy(k).wait()


def call(kernel, outs, limit=24 * MIB, **kw):
    return pl.pallas_call(
        kernel,
        out_shape=outs,
        compiler_params=pltpu.CompilerParams(vmem_limit_bytes=limit),
        **kw,
    )


def shape(dims, dtype):
    return jax.ShapeDtypeStruct(dims, dtype)


def per_device(consts, states, obs_var, relax_rate):
    bx_high, bx_low, bx_high_t, bx_low_t, by, by_t = consts
    field = states[0]
    hbm = pl.BlockSpec(memory_space=pltpu.HBM)
    smem = pl.BlockSpec(memory_space=pltpu.SMEM)
    vmem = pl.BlockSpec(memory_space=pltpu.VMEM)
    width = N // STEPS

    sent = call(
        project_kernel,
        shape((TILES, NEAR, OWN, 2 * ROWS), BF16),
        limit=62 * MIB + MIB // 2,
        in_specs=[hbm, hbm],
        out_specs=vmem,
        scratch_shapes=[
            pltpu.VMEM((STEPS, LEVELS, ROWS, width), BF16),
            pltpu.VMEM((STEPS, width, MODES), BF16),
            pltpu.VMEM((LEVELS * ROWS, MODES), F32),
            pltpu.SemaphoreType.DMA((2 * STEPS,)),
        ],
    )(field, by)
    rows = lax.all_to_all(
        sent.reshape(TILES * NEAR, OWN, 2 * ROWS), ("tile", "near"), 0, 0, tiled=True
    )
    coeffs, copies = call(
        coeffs_kernel,
        (shape((2 * NEAR * OWN, MODES), F32), shape((FAR, 2 * NEAR * OWN, MODES), F32)),
        in_specs=[vmem] * 3,
        out_specs=(vmem, vmem),
        scratch_shapes=[pltpu.VMEM((2 * NEAR * OWN, N), BF16)],
    )(rows.reshape(TILES, NEAR * OWN, 2 * ROWS), bx_high, bx_low)
    gathered = lax.all_to_all(copies, "far", 0, 0, tiled=True)
    back, parts = call(
        nudge_kernel,
        (shape((TILES, NEAR * OWN, 2 * ROWS), BF16), shape((2, TILES, 2 * OWN * OWN), BF16)),
        in_specs=[vmem, vmem, smem, smem, vmem, vmem],
        out_specs=(vmem, vmem),
    )(gathered, coeffs, obs_var, relax_rate, bx_high_t, bx_low_t)
    extra = jnp.broadcast_to(
        jnp.transpose(parts, (1, 0, 2))[:, None, None], (TILES, NEAR, 1, 2, 2 * ROWS)
    )
    out = jnp.concatenate([back.reshape(TILES, NEAR, 4, 2, 2 * ROWS), extra], axis=2)
    got = lax.all_to_all(
        out.reshape(TILES * NEAR, 5, 2, 2 * ROWS), ("tile", "near"), 0, 0, tiled=True
    )
    modes = got[:, :4].reshape(TILES, NEAR, OWN, 2 * ROWS)
    parts = jnp.transpose(got[:, 4], (1, 0, 2))
    nudged, spread = call(
        apply_kernel,
        (shape((LEVELS, ROWS, N), BF16), shape((LEVELS, OWN, MODES), F32)),
        in_specs=[vmem] * 4,
        out_specs=(hbm, vmem),
        scratch_shapes=[
            pltpu.VMEM((LEVELS * ROWS, MODES), BF16),
            pltpu.VMEM((STEPS, LEVELS, ROWS, width), BF16),
            pltpu.VMEM((2 * ROWS, 2 * ROWS), F32),
            pltpu.VMEM((2 * ROWS, 2 * ROWS), F32),
            pltpu.SemaphoreType.DMA((STEPS,)),
        ],
    )(field, modes, parts, by_t)
    return nudged[None], spread


def solution(mesh):
    fine = Mesh(mesh.devices.reshape(FAR, NEAR, TILES), ("far", "near", "tile"))
    rows = P(("far", "near"), None, "tile", None)
    return jax.shard_map(
        functools.partial(per_device, tables()),
        mesh=fine,
        in_specs=(rows, P(), P()),
        out_specs=(rows, P(None, "tile", None)),
        check_vma=False,
    )
```

```python
import functools
import math

import jax
import jax.numpy as jnp
import numpy as np
from jax import lax
from jax.experimental import pallas as pl
from jax.experimental.pallas import tpu as pltpu
from jax.sharding import Mesh, PartitionSpec as P

N = 2048
MODES = 256
LEVELS = 8
MEMBERS = 16
TILES = 32
ROWS = N // TILES
NEAR = 4
FAR = MEMBERS // NEAR
OWN = MODES // TILES
STEPS = 4
CHUNK = OWN + 2
MIB = 1024 * 1024
BF16 = jnp.bfloat16
F32 = jnp.float32


def mode_table():
    mode = np.arange(MODES)[None, :]
    phases = (np.arange(N)[:, None] * ((mode + 1) // 2)) % N
    angles = 2.0 * math.pi / N * phases
    scaled = np.where(mode % 2 == 1, np.sin(angles), np.cos(angles))
    factor = np.where(mode == 0, math.sqrt(1.0 / N), math.sqrt(2.0 / N))
    return (scaled * factor).astype(np.float32)


def tables():
    full = mode_table()
    half = full.astype(BF16)
    first = np.arange(MODES).reshape(TILES, OWN).T.reshape(-1)
    second = np.arange(MODES).reshape(OWN, TILES).T.reshape(-1)
    bx = full[:, first]
    bx_high = bx.astype(BF16)
    bx_low = (bx - bx_high.astype(np.float32)).astype(BF16)
    by = half[:, second]
    flip = lambda a: np.ascontiguousarray(a.T)
    return bx_high, bx_low, flip(bx_high), flip(bx_low), by, flip(by)


def dot(a, b, dims):
    return lax.dot_general(a, b, (dims, ((), ())), preferred_element_type=F32)


def project_kernel(states_ref, by_ref, out_ref, field, table, acc, sems):
    width = N // STEPS

    def copies(k):
        cols = pl.ds(width * k, width)
        return (
            pltpu.make_async_copy(by_ref.at[cols, :], table.at[k], sems.at[2 * k]),
            pltpu.make_async_copy(states_ref.at[:, :, cols], field.at[k], sems.at[2 * k + 1]),
        )

    for k in range(STEPS):
        for c in copies(k):
            c.start()
    for k in range(STEPS):
        for c in copies(k):
            c.wait()
        part = dot(field[k].reshape(LEVELS * ROWS, width), table[k], ((1,), (0,)))
        acc[...] = part if k == 0 else acc[...] + part
    for c in range(NEAR):
        half = acc[2 * ROWS * c : 2 * ROWS * (c + 1), :]
        out_ref[:, c] = half.astype(BF16).T.reshape(TILES, OWN, 2 * ROWS)


def coeffs_kernel(rows_ref, high_ref, low_ref, out_ref, copies_ref, wide):
    for u in range(TILES // 2):
        a, b = rows_ref[2 * u], rows_ref[2 * u + 1]
        cols = pl.ds(2 * ROWS * u, 2 * ROWS)
        wide[: NEAR * OWN, cols] = jnp.concatenate([a[:, :ROWS], b[:, :ROWS]], axis=1)
        wide[NEAR * OWN :, cols] = jnp.concatenate([a[:, ROWS:], b[:, ROWS:]], axis=1)
    x = wide[...]
    coeffs = dot(x, high_ref[...], ((1,), (0,))) + dot(x, low_ref[...], ((1,), (0,)))
    out_ref[...] = coeffs
    for k in range(FAR):
        copies_ref[k] = coeffs


def nudge_kernel(all_ref, own_ref, obs_ref, relax_ref, high_ref, low_ref, sent_ref):
    pair = lax.axis_index("near")
    spreads, misfits = [], []
    for l in range(2):
        def block(ref, k):
            return ref[pl.ds(NEAR * OWN * l + OWN * k, OWN), :]

        driver = block(all_ref.at[0], 0)
        departures = [
            block(all_ref.at[f], k) - driver for f in range(FAR) for k in range(NEAR)
        ]
        mean = sum(departures[1:], departures[0]) * (1.0 / MEMBERS)
        centered = [d - mean for d in departures]
        squares = [c * c for c in centered]
        spread = sum(squares[1:], squares[0]) * (1.0 / MEMBERS)
        gain = relax_ref[2 * pair + l] * spread / (spread + obs_ref[2 * pair + l])
        spreads.append(spread)
        misfits.extend([-gain * (block(own_ref, k) - driver) for k in range(NEAR)])
    misfit = jnp.concatenate(misfits, axis=0)
    high = misfit.astype(BF16)
    low = (misfit - high.astype(F32)).astype(BF16)
    nn = ((1,), (0,))
    count = 2 * NEAR * OWN
    both = dot(jnp.concatenate([high, low], axis=0), high_ref[...], nn)
    back = both[:count] + both[count:] + dot(high, low_ref[...], nn)
    stacked = jnp.concatenate(spreads, axis=0)
    stacked = jnp.concatenate(
        [stacked[:, TILES * k : TILES * (k + 1)] for k in range(OWN)], axis=0
    ).T
    first = stacked.astype(BF16).astype(F32)
    second = stacked - first
    for t in range(TILES):
        half = slice(ROWS * t, ROWS * (t + 1))
        rows = jnp.concatenate([back[: NEAR * OWN, half], back[NEAR * OWN :, half]], axis=1)
        extra = jnp.concatenate([first[t : t + 1], second[t : t + 1]], axis=0)
        pieces = []
        for k in range(NEAR):
            pieces += [rows[OWN * k : OWN * (k + 1)], extra]
        sent_ref[NEAR * CHUNK * t : NEAR * CHUNK * (t + 1), :] = jnp.concatenate(
            pieces, axis=0
        ).astype(BF16)


def apply_kernel(
    states_ref, got_ref, by_ref, out_ref, spread_ref, back, modes, filled, mixed, turned, sems
):
    width = N // STEPS
    for t in range(TILES):
        rows = got_ref[NEAR * CHUNK * t : NEAR * CHUNK * (t + 1), :].astype(F32)
        for c in range(NEAR):
            piece = rows[CHUNK * c : CHUNK * (c + 1)]
            back[c, OWN * t : OWN * (t + 1), :] = piece[:OWN]
            mixed[TILES * c + t : TILES * c + t + 1, :] = piece[OWN : OWN + 1] + piece[OWN + 1 :]
    for c in range(NEAR):
        modes[2 * ROWS * c : 2 * ROWS * (c + 1), :] = back[c].astype(BF16).T

    def copy(k):
        cols = pl.ds(width * k, width)
        return pltpu.make_async_copy(filled.at[k], out_ref.at[:, :, cols], sems.at[k])

    for k in range(STEPS):
        cols = slice(width * k, width * (k + 1))
        increment = dot(modes[...], by_ref[:, cols], ((1,), (0,)))
        field = states_ref[:, :, cols].astype(F32)
        filled[k] = (field + increment.reshape(LEVELS, ROWS, width)).astype(BF16)
        copy(k).start()

    turned[...] = mixed[...].T
    for l in range(2):
        strips = [turned[pl.ds(OWN * l + k, OWN, stride=2 * OWN), :] for k in range(OWN)]
        for c in range(NEAR):
            spread_ref[2 * c + l] = jnp.concatenate(
                [s[:, TILES * c : TILES * (c + 1)] for s in strips], axis=1
            )
    for k in range(STEPS):
        copy(k).wait()


def call(kernel, outs, limit=24 * MIB, **kw):
    return pl.pallas_call(
        kernel,
        out_shape=outs,
        compiler_params=pltpu.CompilerParams(vmem_limit_bytes=limit),
        **kw,
    )


def shape(dims, dtype):
    return jax.ShapeDtypeStruct(dims, dtype)


def per_device(consts, states, obs_var, relax_rate):
    bx_high, bx_low, bx_high_t, bx_low_t, by, by_t = consts
    field = states[0]
    hbm = pl.BlockSpec(memory_space=pltpu.HBM)
    smem = pl.BlockSpec(memory_space=pltpu.SMEM)
    vmem = pl.BlockSpec(memory_space=pltpu.VMEM)
    width = N // STEPS

    sent = call(
        project_kernel,
        shape((TILES, NEAR, OWN, 2 * ROWS), BF16),
        in_specs=[hbm, hbm],
        out_specs=vmem,
        scratch_shapes=[
            pltpu.VMEM((STEPS, LEVELS, ROWS, width), BF16),
            pltpu.VMEM((STEPS, width, MODES), BF16),
            pltpu.VMEM((LEVELS * ROWS, MODES), F32),
            pltpu.SemaphoreType.DMA((2 * STEPS,)),
        ],
    )(*(pltpu.with_memory_space_constraint(x, pltpu.HBM) for x in (field, by)))
    rows = lax.all_to_all(
        sent.reshape(TILES * NEAR, OWN, 2 * ROWS), ("tile", "near"), 0, 0, tiled=True
    )
    coeffs, copies = call(
        coeffs_kernel,
        (shape((2 * NEAR * OWN, MODES), F32), shape((FAR, 2 * NEAR * OWN, MODES), F32)),
        in_specs=[vmem] * 3,
        out_specs=(vmem, vmem),
        scratch_shapes=[pltpu.VMEM((2 * NEAR * OWN, N), BF16)],
    )(rows.reshape(TILES, NEAR * OWN, 2 * ROWS), bx_high, bx_low)
    gathered = lax.all_to_all(copies, "far", 0, 0, tiled=True)
    sent = call(
        nudge_kernel,
        shape((TILES * NEAR * CHUNK, 2 * ROWS), BF16),
        in_specs=[vmem, vmem, smem, smem, vmem, vmem],
        out_specs=vmem,
    )(gathered, coeffs, obs_var, relax_rate, bx_high_t, bx_low_t)
    got = lax.all_to_all(
        sent.reshape(TILES * NEAR, CHUNK // 2, 2, 2 * ROWS), ("tile", "near"), 0, 0, tiled=True
    )
    nudged, spread = call(
        apply_kernel,
        (shape((LEVELS, ROWS, N), BF16), shape((LEVELS, OWN, MODES), F32)),
        in_specs=[vmem] * 3,
        out_specs=(hbm, vmem),
        scratch_shapes=[
            pltpu.VMEM((NEAR, MODES, 2 * ROWS), F32),
            pltpu.VMEM((LEVELS * ROWS, MODES), BF16),
            pltpu.VMEM((STEPS, LEVELS, ROWS, width), BF16),
            pltpu.VMEM((2 * ROWS, 2 * ROWS), F32),
            pltpu.VMEM((2 * ROWS, 2 * ROWS), F32),
            pltpu.SemaphoreType.DMA((STEPS,)),
        ],
    )(field, got.reshape(TILES * NEAR * CHUNK, 2 * ROWS), by_t)
    return nudged[None], spread


def solution(mesh):
    fine = Mesh(mesh.devices.reshape(FAR, NEAR, TILES), ("far", "near", "tile"))
    rows = P(("far", "near"), None, "tile", None)
    return jax.shard_map(
        functools.partial(per_device, tables()),
        mesh=fine,
        in_specs=(rows, P(), P()),
        out_specs=(rows, P(None, "tile", None)),
        check_vma=False,
    )
```

```python
import functools
import math

import jax
import jax.numpy as jnp
import numpy as np
from jax import lax
from jax.experimental import pallas as pl
from jax.experimental.pallas import tpu as pltpu
from jax.sharding import Mesh, PartitionSpec as P

N = 2048
MODES = 256
LEVELS = 8
MEMBERS = 16
TILES = 32
ROWS = N // TILES
NEAR = 4
FAR = MEMBERS // NEAR
OWN = MODES // TILES
STEPS = 4
HALF = N // 2
WIDTH = HALF // STEPS
CHUNK = OWN + 2
MIB = 1024 * 1024
BF16 = jnp.bfloat16
F32 = jnp.float32


def mode_table():
    mode = np.arange(MODES)[None, :]
    phases = (np.arange(N)[:, None] * ((mode + 1) // 2)) % N
    angles = 2.0 * math.pi / N * phases
    scaled = np.where(mode % 2 == 1, np.sin(angles), np.cos(angles))
    factor = np.where(mode == 0, math.sqrt(1.0 / N), math.sqrt(2.0 / N))
    return (scaled * factor).astype(np.float32)


def tables():
    full = mode_table()[:HALF]
    high = full.astype(BF16)
    low = (full - high.astype(np.float32)).astype(BF16)
    first = np.arange(MODES).reshape(TILES, OWN).T.reshape(-1)
    second = np.arange(MODES).reshape(OWN, TILES).T.reshape(-1)
    flip = lambda a: np.ascontiguousarray(a.T)
    bx_high, bx_low, by = high[:, first], low[:, first], high[:, second]
    return bx_high, bx_low, flip(bx_high), flip(bx_low), by, flip(by)


def signs(major, minor):
    column = lax.broadcasted_iota(jnp.int32, (1, MODES), 1)
    mode = major * (column % minor) + column // minor
    return (1 - 2 * ((mode + 1) // 2 % 2)).astype(F32)


def dot(a, b, dims):
    return lax.dot_general(a, b, (dims, ((), ())), preferred_element_type=F32)


def project_kernel(states_ref, by_ref, out_ref, field, table, acc, sems):
    def copies(k):
        rows = pl.ds(WIDTH * k, WIDTH)
        yield pltpu.make_async_copy(by_ref.at[rows, :], table.at[k], sems.at[3 * k])
        for h in range(2):
            cols = pl.ds(HALF * h + WIDTH * k, WIDTH)
            yield pltpu.make_async_copy(
                states_ref.at[:, :, cols], field.at[k, h], sems.at[3 * k + 1 + h]
            )

    for k in range(STEPS):
        for c in copies(k):
            c.start()
    for k in range(STEPS):
        for c in copies(k):
            c.wait()
        for h in range(2):
            part = dot(field[k, h].reshape(LEVELS * ROWS, WIDTH), table[k], ((1,), (0,)))
            rows = slice(LEVELS * ROWS * h, LEVELS * ROWS * (h + 1))
            acc[rows, :] = part if k == 0 else acc[rows, :] + part
    sign = signs(TILES, OWN)
    for c in range(NEAR):
        lower = acc[2 * ROWS * c : 2 * ROWS * (c + 1), :]
        upper = acc[LEVELS * ROWS + 2 * ROWS * c : LEVELS * ROWS + 2 * ROWS * (c + 1), :]
        half = (lower + sign * upper).astype(BF16)
        out_ref[:, c] = half.T.reshape(TILES, OWN, 2 * ROWS)


def coeffs_kernel(rows_ref, high_ref, low_ref, out_ref, copies_ref, wide):
    count = NEAR * OWN
    for u in range(TILES // 2):
        a, b = rows_ref[2 * u], rows_ref[2 * u + 1]
        row = 2 * count * (u // (TILES // 4))
        cols = pl.ds(2 * ROWS * (u % (TILES // 4)), 2 * ROWS)
        wide[row : row + count, cols] = jnp.concatenate([a[:, :ROWS], b[:, :ROWS]], axis=1)
        wide[row + count : row + 2 * count, cols] = jnp.concatenate(
            [a[:, ROWS:], b[:, ROWS:]], axis=1
        )
    x = wide[...]
    both = dot(x, high_ref[...], ((1,), (0,))) + dot(x, low_ref[...], ((1,), (0,)))
    coeffs = both[: 2 * count] + signs(OWN, TILES) * both[2 * count :]
    out_ref[...] = coeffs
    for k in range(FAR):
        copies_ref[k] = coeffs


def nudge_kernel(all_ref, own_ref, obs_ref, relax_ref, high_ref, low_ref, sent_ref):
    pair = lax.axis_index("near")
    spreads, misfits = [], []
    for l in range(2):
        def block(ref, k):
            return ref[pl.ds(NEAR * OWN * l + OWN * k, OWN), :]

        driver = block(all_ref.at[0], 0)
        departures = [
            block(all_ref.at[f], k) - driver for f in range(FAR) for k in range(NEAR)
        ]
        mean = sum(departures[1:], departures[0]) * (1.0 / MEMBERS)
        centered = [d - mean for d in departures]
        squares = [c * c for c in centered]
        spread = sum(squares[1:], squares[0]) * (1.0 / MEMBERS)
        gain = relax_ref[2 * pair + l] * spread / (spread + obs_ref[2 * pair + l])
        spreads.append(spread)
        misfits.extend([-gain * (block(own_ref, k) - driver) for k in range(NEAR)])
    misfit = jnp.concatenate(misfits, axis=0)
    high = misfit.astype(BF16)
    low = (misfit - high.astype(F32)).astype(BF16)
    nn = ((1,), (0,))
    count = 2 * NEAR * OWN
    sign = signs(OWN, TILES).astype(BF16)
    high = jnp.concatenate([high, high * sign], axis=0)
    low = jnp.concatenate([low, low * sign], axis=0)
    both = dot(jnp.concatenate([high, low], axis=0), high_ref[...], nn)
    back = both[: 2 * count] + both[2 * count :] + dot(high, low_ref[...], nn)
    stacked = jnp.concatenate(spreads, axis=0)
    stacked = jnp.concatenate(
        [stacked[:, TILES * k : TILES * (k + 1)] for k in range(OWN)], axis=0
    ).T
    first = stacked.astype(BF16).astype(F32)
    second = stacked - first
    for t in range(TILES):
        row, col = divmod(t, TILES // 2)
        block = back[count * row : count * (row + 1), ROWS * col : ROWS * (col + 1)]
        rows = jnp.concatenate([block[: NEAR * OWN], block[NEAR * OWN :]], axis=1)
        extra = jnp.concatenate([first[t : t + 1], second[t : t + 1]], axis=0)
        pieces = []
        for k in range(NEAR):
            pieces += [rows[OWN * k : OWN * (k + 1)], extra]
        sent_ref[NEAR * CHUNK * t : NEAR * CHUNK * (t + 1), :] = jnp.concatenate(
            pieces, axis=0
        ).astype(BF16)


def apply_kernel(
    states_ref, got_ref, by_ref, out_ref, spread_ref, back, filled, mixed, turned, sems
):
    def copy(c):
        levels = pl.ds(2 * c, 2)
        return pltpu.make_async_copy(filled.at[levels], out_ref.at[levels], sems.at[c])

    sign = signs(TILES, OWN).astype(BF16)
    for c in range(NEAR):
        for t in range(TILES):
            row = CHUNK * (NEAR * t + c)
            piece = got_ref[row : row + CHUNK, :].astype(F32)
            back[OWN * t : OWN * (t + 1), :] = piece[:OWN]
            mixed[TILES * c + t : TILES * c + t + 1, :] = piece[OWN : OWN + 1] + piece[OWN + 1 :]
        modes = back[...].astype(BF16).T
        for h in range(2):
            cols = slice(HALF * h, HALF * (h + 1))
            increment = dot(modes if h == 0 else modes * sign, by_ref[...], ((1,), (0,)))
            field = states_ref[2 * c : 2 * c + 2, :, cols].astype(F32)
            total = field + increment.reshape(2, ROWS, HALF)
            filled[2 * c : 2 * c + 2, :, cols] = total.astype(BF16)
        copy(c).start()
    turned[...] = mixed[...].T
    for l in range(2):
        strips = [turned[pl.ds(OWN * l + k, OWN, stride=2 * OWN), :] for k in range(OWN)]
        for c in range(NEAR):
            spread_ref[2 * c + l] = jnp.concatenate(
                [s[:, TILES * c : TILES * (c + 1)] for s in strips], axis=1
            )
    for c in range(NEAR):
        copy(c).wait()


def call(kernel, outs, limit=24 * MIB, **kw):
    return pl.pallas_call(
        kernel,
        out_shape=outs,
        compiler_params=pltpu.CompilerParams(vmem_limit_bytes=limit),
        **kw,
    )


def shape(dims, dtype):
    return jax.ShapeDtypeStruct(dims, dtype)


def per_device(consts, states, obs_var, relax_rate):
    bx_high, bx_low, bx_high_t, bx_low_t, by, by_t = consts
    field = states[0]
    hbm = pl.BlockSpec(memory_space=pltpu.HBM)
    smem = pl.BlockSpec(memory_space=pltpu.SMEM)
    vmem = pl.BlockSpec(memory_space=pltpu.VMEM)

    sent = call(
        project_kernel,
        shape((TILES, NEAR, OWN, 2 * ROWS), BF16),
        in_specs=[hbm, hbm],
        out_specs=vmem,
        scratch_shapes=[
            pltpu.VMEM((STEPS, 2, LEVELS, ROWS, WIDTH), BF16),
            pltpu.VMEM((STEPS, WIDTH, MODES), BF16),
            pltpu.VMEM((2 * LEVELS * ROWS, MODES), F32),
            pltpu.SemaphoreType.DMA((3 * STEPS,)),
        ],
    )(*(pltpu.with_memory_space_constraint(x, pltpu.HBM) for x in (field, by)))
    rows = lax.all_to_all(
        sent.reshape(TILES * NEAR, OWN, 2 * ROWS), ("tile", "near"), 0, 0, tiled=True
    )
    coeffs, copies = call(
        coeffs_kernel,
        (shape((2 * NEAR * OWN, MODES), F32), shape((FAR, 2 * NEAR * OWN, MODES), F32)),
        in_specs=[vmem] * 3,
        out_specs=(vmem, vmem),
        scratch_shapes=[pltpu.VMEM((4 * NEAR * OWN, HALF), BF16)],
    )(rows.reshape(TILES, NEAR * OWN, 2 * ROWS), bx_high, bx_low)
    gathered = lax.all_to_all(copies, "far", 0, 0, tiled=True)
    sent = call(
        nudge_kernel,
        shape((TILES * NEAR * CHUNK, 2 * ROWS), BF16),
        in_specs=[vmem, vmem, smem, smem, vmem, vmem],
        out_specs=vmem,
    )(gathered, coeffs, obs_var, relax_rate, bx_high_t, bx_low_t)
    got = lax.all_to_all(
        sent.reshape(TILES * NEAR, CHUNK // 2, 2, 2 * ROWS), ("tile", "near"), 0, 0, tiled=True
    )
    nudged, spread = call(
        apply_kernel,
        (shape((LEVELS, ROWS, N), BF16), shape((LEVELS, OWN, MODES), F32)),
        in_specs=[vmem] * 3,
        out_specs=(hbm, vmem),
        scratch_shapes=[
            pltpu.VMEM((MODES, 2 * ROWS), F32),
            pltpu.VMEM((LEVELS, ROWS, N), BF16),
            pltpu.VMEM((2 * ROWS, 2 * ROWS), F32),
            pltpu.VMEM((2 * ROWS, 2 * ROWS), F32),
            pltpu.SemaphoreType.DMA((NEAR,)),
        ],
    )(field, got.reshape(TILES * NEAR * CHUNK, 2 * ROWS), by_t)
    return nudged[None], spread


def solution(mesh):
    fine = Mesh(mesh.devices.reshape(FAR, NEAR, TILES), ("far", "near", "tile"))
    rows = P(("far", "near"), None, "tile", None)
    return jax.shard_map(
        functools.partial(per_device, tables()),
        mesh=fine,
        in_specs=(rows, P(), P()),
        out_specs=(rows, P(None, "tile", None)),
        check_vma=False,
    )
```

```python
import functools
import math

import jax
import jax.numpy as jnp
import numpy as np
from jax import lax
from jax.experimental import pallas as pl
from jax.experimental.pallas import tpu as pltpu
from jax.sharding import Mesh, PartitionSpec as P

N = 2048
MODES = 256
LEVELS = 8
MEMBERS = 16
TILES = 32
ROWS = N // TILES
NEAR = 4
FAR = MEMBERS // NEAR
OWN = MODES // TILES
STEPS = 4
HALF = N // 2
WIDTH = HALF // STEPS
SLOTS = 32
RANK = 20
GROUP = 4
SIDE = MODES // GROUP
CHUNK = GROUP + 2
PART = NEAR * GROUP
MIB = 1024 * 1024
BF16 = jnp.bfloat16
F32 = jnp.float32


def mode_table():
    mode = np.arange(MODES)[None, :]
    phases = (np.arange(N)[:, None] * ((mode + 1) // 2)) % N
    angles = 2.0 * math.pi / N * phases
    scaled = np.where(mode % 2 == 1, np.sin(angles), np.cos(angles))
    factor = np.where(mode == 0, math.sqrt(1.0 / N), math.sqrt(2.0 / N))
    return scaled * factor


def row_basis():
    n = np.arange(ROWS)
    centre = ((ROWS - 1 - 2 * n) / 2.0) ** 2 * math.cos(math.pi * MODES / N)
    beside = n[1:] * (ROWS - n[1:]) / 2.0
    vectors = np.linalg.eigh(np.diag(centre) + np.diag(beside, 1) + np.diag(beside, -1))[1]
    basis = vectors[:, ::-1][:, :RANK]
    return basis * np.sign(basis[0])


def split(table):
    high = table.astype(np.float32).astype(BF16)
    return high, (table - high.astype(np.float64)).astype(np.float32).astype(BF16)


def tables():
    full = mode_table()
    flip = lambda a: np.ascontiguousarray(a.T)
    first = np.arange(MODES).reshape(TILES, OWN).T.reshape(-1)
    second = np.arange(MODES).reshape(GROUP, SIDE).T.reshape(-1)
    slots = np.concatenate([np.arange(RANK), np.arange(SLOTS - RANK)])
    basis = row_basis()
    blocks = full.reshape(TILES, ROWS, MODES)
    modes = np.stack(
        [(blocks * basis[:, k][None, :, None]).sum(axis=1) for k in range(RANK)], axis=1
    )
    bx_high, bx_low = split(modes[:, slots][:, :, first].reshape(TILES * SLOTS, MODES))
    narrow = np.kron(np.eye(GROUP), basis[:, slots].T)
    narrow_high, narrow_low = split(narrow)
    by = full[:HALF].astype(np.float32).astype(BF16)[:, second]
    narrow_both = np.concatenate([narrow_high, narrow_low], axis=0)
    spread_both = np.concatenate([flip(narrow_high), flip(narrow_low)], axis=0)
    return bx_high, bx_low, flip(bx_high), flip(bx_low), by, flip(by), narrow_both, spread_both


def signs(major, minor):
    column = lax.broadcasted_iota(jnp.int32, (1, MODES), 1)
    mode = major * (column % minor) + column // minor
    return (1 - 2 * ((mode + 1) // 2 % 2)).astype(F32)


def dot(a, b, dims):
    return lax.dot_general(a, b, (dims, ((), ())), preferred_element_type=F32)


def parts(values):
    high = values.astype(BF16)
    return high, (values - high.astype(F32)).astype(BF16)


def low_slots(values, axis):
    slot = lax.broadcasted_iota(jnp.int32, values.shape, axis) % SLOTS
    rounded = values.astype(BF16).astype(F32)
    return jnp.where(slot < RANK, rounded, values - rounded)


def project_kernel(states_ref, by_ref, narrow_ref, out_ref, field, table, small, acc, sems):
    last = pltpu.make_async_copy(narrow_ref, small, sems.at[3 * STEPS])

    def copies(k):
        rows = pl.ds(WIDTH * k, WIDTH)
        yield pltpu.make_async_copy(by_ref.at[rows, :], table.at[k], sems.at[3 * k])
        for h in range(2):
            cols = pl.ds(HALF * h + WIDTH * k, WIDTH)
            yield pltpu.make_async_copy(
                states_ref.at[:, :, cols], field.at[k, h], sems.at[3 * k + 1 + h]
            )

    for k in range(STEPS):
        for c in copies(k):
            c.start()
    last.start()
    for k in range(STEPS):
        for c in copies(k):
            c.wait()
        for h in range(2):
            part = dot(field[k, h].reshape(LEVELS * ROWS, WIDTH), table[k], ((1,), (0,)))
            rows = slice(LEVELS * ROWS * h, LEVELS * ROWS * (h + 1))
            acc[rows, :] = part if k == 0 else acc[rows, :] + part
    last.wait()
    sign = signs(SIDE, GROUP)
    count = GROUP * SLOTS
    sides = []
    for c in range(2):
        lower = acc[GROUP * ROWS * c : GROUP * ROWS * (c + 1), :]
        upper = acc[GROUP * ROWS * (c + 2) : GROUP * ROWS * (c + 3), :]
        high, low = parts(lower + sign * upper)
        both = dot(small[...], high, ((1,), (0,)))
        narrow = both[:count] + both[count:] + dot(small[:count, :], low, ((1,), (0,)))
        sides.append(low_slots(narrow, 0).T)
    for r in range(SIDE // 2):
        rows = []
        for k in range(2):
            for side in sides:
                rows.append(side[GROUP * (2 * r + k) : GROUP * (2 * r + k + 1)])
        out_ref[4 * GROUP * r : 4 * GROUP * (r + 1), :] = jnp.concatenate(rows, axis=0).astype(BF16)


def coeffs_kernel(rows_ref, high_ref, low_ref, out_ref, copies_ref, wide):
    lanes = GROUP * SLOTS
    for u in range(TILES // GROUP):
        pieces = [rows_ref[PART * (GROUP * u + k) : PART * (GROUP * u + k + 1), :] for k in range(GROUP)]
        for l in range(GROUP):
            wide[PART * l : PART * (l + 1), lanes * u : lanes * (u + 1)] = jnp.concatenate(
                [p[:, SLOTS * l : SLOTS * (l + 1)] for p in pieces], axis=1
            )
    x = wide[...]
    coeffs = dot(x, high_ref[...], ((1,), (0,))) + dot(x, low_ref[...], ((1,), (0,)))
    coeffs = swap_rows(coeffs)
    out_ref[...] = coeffs
    for k in range(FAR):
        copies_ref[k] = coeffs


def swap_rows(values):
    return jnp.concatenate(
        [
            values[PART * l + GROUP * k : PART * l + GROUP * (k + 1)]
            for k in range(GROUP)
            for l in range(NEAR)
        ],
        axis=0,
    )


def nudge_kernel(all_ref, own_ref, obs_ref, relax_ref, high_ref, low_ref, sent_ref):
    base = GROUP * (lax.axis_index("near") % 2)
    level = lax.broadcasted_iota(jnp.int32, (PART, MODES), 0) // GROUP
    obs = jnp.zeros((PART, MODES), F32)
    relax = jnp.zeros((PART, MODES), F32)
    for l in range(GROUP):
        obs = jnp.where(level == l, obs_ref[base + l], obs)
        relax = jnp.where(level == l, relax_ref[base + l], relax)
    members = [slice(PART * k, PART * (k + 1)) for k in range(NEAR)]
    driver = all_ref[0, members[0], :]
    departures = [all_ref[f, m, :] - driver for f in range(FAR) for m in members]
    mean = sum(departures[1:], departures[0]) * (1.0 / MEMBERS)
    squares = [(d - mean) * (d - mean) for d in departures]
    spread = sum(squares[1:], squares[0]) * (1.0 / MEMBERS)
    gain = relax * spread / (spread + obs)
    misfit = jnp.concatenate([-gain * (own_ref[m, :] - driver) for m in members], axis=0)
    high, low = parts(swap_rows(misfit))
    count = NEAR * PART
    both = dot(jnp.concatenate([high, low], axis=0), high_ref[...], ((1,), (0,)))
    back = both[:count] + both[count:] + dot(high, low_ref[...], ((1,), (0,)))
    back = low_slots(back, 1)
    stacked = jnp.concatenate(
        [spread[:, TILES * k : TILES * (k + 1)] for k in range(OWN)], axis=0
    ).T
    first = stacked.astype(BF16).astype(F32)
    second = stacked - first
    for t in range(TILES):
        cols = slice(SLOTS * t, SLOTS * (t + 1))
        rows = jnp.concatenate([back[PART * l : PART * (l + 1), cols] for l in range(GROUP)], axis=1)
        extra = jnp.concatenate([first[t : t + 1], second[t : t + 1]], axis=0)
        pieces = []
        for k in range(NEAR):
            pieces += [rows[GROUP * k : GROUP * (k + 1)], extra]
        sent_ref[NEAR * CHUNK * t : NEAR * CHUNK * (t + 1), :] = jnp.concatenate(
            pieces, axis=0
        ).astype(BF16)


def apply_kernel(
    states_ref, got_ref, by_ref, wide_ref, out_ref, spread_ref, back, filled, mixed, turned, sems
):
    def copy(c, h):
        part = (pl.ds(GROUP * c, GROUP), slice(None), pl.ds(HALF * h, HALF))
        return pltpu.make_async_copy(filled.at[part], out_ref.at[part], sems.at[2 * c + h])

    for t in range(TILES):
        rows = got_ref[NEAR * CHUNK * t : NEAR * CHUNK * (t + 1), :].astype(F32)
        for k in range(NEAR):
            piece = rows[CHUNK * k : CHUNK * (k + 1)]
            r, c = 2 * t + k // 2, k % 2
            back[c, GROUP * r : GROUP * (r + 1), :] = piece[:GROUP]
            mixed[SIDE * c + r : SIDE * c + r + 1, :] = piece[GROUP : GROUP + 1] + piece[GROUP + 1 :]
    sign = signs(SIDE, GROUP).astype(BF16)
    count = GROUP * ROWS
    for c in range(2):
        both = dot(wide_ref[...], back[c].astype(BF16).T, ((1,), (0,)))
        modes = (both[:count] + both[count:]).astype(BF16)
        for h in range(2):
            cols = slice(HALF * h, HALF * (h + 1))
            increment = dot(modes if h == 0 else modes * sign, by_ref[...], ((1,), (0,)))
            field = states_ref[GROUP * c : GROUP * (c + 1), :, cols].astype(F32)
            total = field + increment.reshape(GROUP, ROWS, HALF)
            filled[GROUP * c : GROUP * (c + 1), :, cols] = total.astype(BF16)
            copy(c, h).start()
    turned[...] = mixed[...].T
    for l in range(GROUP):
        strips = [turned[pl.ds(GROUP * l + k, OWN, stride=PART), :] for k in range(GROUP)]
        for c in range(2):
            spread_ref[GROUP * c + l] = jnp.concatenate(
                [s[:, SIDE * c : SIDE * (c + 1)] for s in strips], axis=1
            )
    for c in range(2):
        for h in range(2):
            copy(c, h).wait()


def call(kernel, outs, limit=24 * MIB, **kw):
    return pl.pallas_call(
        kernel,
        out_shape=outs,
        compiler_params=pltpu.CompilerParams(vmem_limit_bytes=limit),
        **kw,
    )


def shape(dims, dtype):
    return jax.ShapeDtypeStruct(dims, dtype)


def per_device(consts, states, obs_var, relax_rate):
    bx_high, bx_low, bx_high_t, bx_low_t, by, by_t, narrow, widen = consts
    field = states[0]
    hbm = pl.BlockSpec(memory_space=pltpu.HBM)
    smem = pl.BlockSpec(memory_space=pltpu.SMEM)
    vmem = pl.BlockSpec(memory_space=pltpu.VMEM)
    devices, lanes, columns = TILES * NEAR, GROUP * SLOTS, NEAR * PART

    def exchange(rows):
        chunks = rows.reshape(devices, rows.shape[0] // (2 * devices), 2, lanes)
        return lax.all_to_all(chunks, ("tile", "near"), 0, 0, tiled=True).reshape(rows.shape)

    sent = call(
        project_kernel,
        shape((devices * GROUP, lanes), BF16),
        in_specs=[hbm] * 3,
        out_specs=vmem,
        scratch_shapes=[
            pltpu.VMEM((STEPS, 2, LEVELS, ROWS, WIDTH), BF16),
            pltpu.VMEM((STEPS, WIDTH, MODES), BF16),
            pltpu.VMEM((2 * lanes, GROUP * ROWS), BF16),
            pltpu.VMEM((2 * LEVELS * ROWS, MODES), F32),
            pltpu.SemaphoreType.DMA((3 * STEPS + 1,)),
        ],
    )(*(pltpu.with_memory_space_constraint(x, pltpu.HBM) for x in (field, by, narrow)))
    coeffs, copies = call(
        coeffs_kernel,
        (shape((columns, MODES), F32), shape((FAR, columns, MODES), F32)),
        in_specs=[vmem] * 3,
        out_specs=(vmem, vmem),
        scratch_shapes=[pltpu.VMEM((columns, TILES * SLOTS), BF16)],
    )(exchange(sent), bx_high, bx_low)
    gathered = lax.all_to_all(copies, "far", 0, 0, tiled=True)
    sent = call(
        nudge_kernel,
        shape((devices * CHUNK, lanes), BF16),
        in_specs=[vmem, vmem, smem, smem, vmem, vmem],
        out_specs=vmem,
    )(gathered, coeffs, obs_var, relax_rate, bx_high_t, bx_low_t)
    nudged, spread = call(
        apply_kernel,
        (shape((LEVELS, ROWS, N), BF16), shape((LEVELS, OWN, MODES), F32)),
        in_specs=[vmem] * 4,
        out_specs=(hbm, vmem),
        scratch_shapes=[
            pltpu.VMEM((2, MODES, lanes), F32),
            pltpu.VMEM((LEVELS, ROWS, N), BF16),
            pltpu.VMEM((2 * SIDE, lanes), F32),
            pltpu.VMEM((lanes, 2 * SIDE), F32),
            pltpu.SemaphoreType.DMA((4,)),
        ],
    )(field, exchange(sent), by_t, widen)
    return nudged[None], spread


def solution(mesh):
    fine = Mesh(mesh.devices.reshape(FAR, NEAR, TILES), ("far", "near", "tile"))
    rows = P(("far", "near"), None, "tile", None)
    return jax.shard_map(
        functools.partial(per_device, tables()),
        mesh=fine,
        in_specs=(rows, P(), P()),
        out_specs=(rows, P(None, "tile", None)),
        check_vma=False,
    )
```

```python
import functools
import math

import jax
import jax.numpy as jnp
import numpy as np
from jax import lax
from jax.experimental import pallas as pl
from jax.experimental.pallas import tpu as pltpu
from jax.sharding import Mesh, PartitionSpec as P

N = 2048
MODES = 256
LEVELS = 8
MEMBERS = 16
TILES = 32
ROWS = N // TILES
NEAR = 4
FAR = MEMBERS // NEAR
OWN = MODES // TILES
STEPS = 4
HALF = N // 2
WIDTH = HALF // STEPS
SLOTS = 32
RANK = 20
GROUP = 4
SIDE = MODES // GROUP
CHUNK = GROUP + 2
PART = NEAR * GROUP
MIB = 1024 * 1024
BF16 = jnp.bfloat16
F32 = jnp.float32


def mode_table():
    mode = np.arange(MODES)[None, :]
    phases = (np.arange(N)[:, None] * ((mode + 1) // 2)) % N
    angles = 2.0 * math.pi / N * phases
    scaled = np.where(mode % 2 == 1, np.sin(angles), np.cos(angles))
    factor = np.where(mode == 0, math.sqrt(1.0 / N), math.sqrt(2.0 / N))
    return scaled * factor


def row_basis():
    n = np.arange(ROWS)
    centre = ((ROWS - 1 - 2 * n) / 2.0) ** 2 * math.cos(math.pi * MODES / N)
    beside = n[1:] * (ROWS - n[1:]) / 2.0
    vectors = np.linalg.eigh(np.diag(centre) + np.diag(beside, 1) + np.diag(beside, -1))[1]
    basis = vectors[:, ::-1][:, :RANK]
    return basis * np.sign(basis[0])


def split(table):
    high = table.astype(np.float32).astype(BF16)
    return high, (table - high.astype(np.float64)).astype(np.float32).astype(BF16)


def tables():
    full = mode_table()
    flip = lambda a: np.ascontiguousarray(a.T)
    first = np.arange(MODES).reshape(TILES, OWN).T.reshape(-1)
    second = np.arange(MODES).reshape(GROUP, SIDE).T.reshape(-1)
    slots = np.concatenate([np.arange(RANK), np.arange(SLOTS - RANK)])
    basis = row_basis()
    blocks = full.reshape(TILES, ROWS, MODES)
    modes = np.stack(
        [(blocks * basis[:, k][None, :, None]).sum(axis=1) for k in range(RANK)], axis=1
    )
    bx_high, bx_low = split(modes[:, slots][:, :, first].reshape(TILES * SLOTS, MODES))
    narrow = np.kron(np.eye(GROUP), basis[:, slots].T)
    narrow_high, narrow_low = split(narrow)
    by = full[:HALF].astype(np.float32).astype(BF16)[:, second]
    narrow_both = np.concatenate([narrow_high, narrow_low], axis=0)
    spread_both = np.concatenate([flip(narrow_high), flip(narrow_low)], axis=0)
    return bx_high, bx_low, flip(bx_high), flip(bx_low), by, flip(by), narrow_both, spread_both


def signs(major, minor):
    column = lax.broadcasted_iota(jnp.int32, (1, MODES), 1)
    mode = major * (column % minor) + column // minor
    return (1 - 2 * ((mode + 1) // 2 % 2)).astype(F32)


def dot(a, b, dims):
    return lax.dot_general(a, b, (dims, ((), ())), preferred_element_type=F32)


def parts(values):
    high = values.astype(BF16)
    return high, (values - high.astype(F32)).astype(BF16)


def low_slots(values, axis):
    slot = lax.broadcasted_iota(jnp.int32, values.shape, axis) % SLOTS
    rounded = values.astype(BF16).astype(F32)
    return jnp.where(slot < RANK, rounded, values - rounded)


def project_kernel(states_ref, by_ref, narrow_ref, out_ref, field, table, small, acc, sems):
    last = pltpu.make_async_copy(narrow_ref, small, sems.at[3 * STEPS])

    def copies(k):
        rows = pl.ds(WIDTH * k, WIDTH)
        yield pltpu.make_async_copy(by_ref.at[rows, :], table.at[k], sems.at[3 * k])
        for h in range(2):
            cols = pl.ds(HALF * h + WIDTH * k, WIDTH)
            yield pltpu.make_async_copy(
                states_ref.at[:, :, cols], field.at[k, h], sems.at[3 * k + 1 + h]
            )

    for k in range(STEPS):
        for c in copies(k):
            c.start()
    last.start()
    for k in range(STEPS):
        for c in copies(k):
            c.wait()
        for h in range(2):
            part = dot(field[k, h].reshape(LEVELS * ROWS, WIDTH), table[k], ((1,), (0,)))
            rows = slice(LEVELS * ROWS * h, LEVELS * ROWS * (h + 1))
            acc[rows, :] = part if k == 0 else acc[rows, :] + part
    last.wait()
    sign = signs(SIDE, GROUP)
    count = GROUP * SLOTS
    sides = []
    for c in range(2):
        lower = acc[GROUP * ROWS * c : GROUP * ROWS * (c + 1), :]
        upper = acc[GROUP * ROWS * (c + 2) : GROUP * ROWS * (c + 3), :]
        high, low = parts(lower + sign * upper)
        both = dot(small[...], high, ((1,), (0,)))
        narrow = both[:count] + both[count:] + dot(small[:count, :], low, ((1,), (0,)))
        sides.append(low_slots(narrow, 0).T)
    for r in range(SIDE // 2):
        rows = []
        for k in range(2):
            for side in sides:
                rows.append(side[GROUP * (2 * r + k) : GROUP * (2 * r + k + 1)])
        out_ref[4 * GROUP * r : 4 * GROUP * (r + 1), :] = jnp.concatenate(rows, axis=0).astype(BF16)


def coeffs_kernel(rows_ref, high_ref, low_ref, out_ref, copies_ref, wide):
    lanes = GROUP * SLOTS
    for u in range(TILES // GROUP):
        pieces = [rows_ref[PART * (GROUP * u + k) : PART * (GROUP * u + k + 1), :] for k in range(GROUP)]
        for l in range(GROUP):
            wide[PART * l : PART * (l + 1), lanes * u : lanes * (u + 1)] = jnp.concatenate(
                [p[:, SLOTS * l : SLOTS * (l + 1)] for p in pieces], axis=1
            )
    x = wide[...]
    coeffs = dot(x, high_ref[...], ((1,), (0,))) + dot(x, low_ref[...], ((1,), (0,)))
    coeffs = swap_rows(coeffs)
    out_ref[...] = coeffs
    for k in range(FAR):
        copies_ref[k] = coeffs


def swap_rows(values):
    return jnp.concatenate(
        [
            values[PART * l + GROUP * k : PART * l + GROUP * (k + 1)]
            for k in range(GROUP)
            for l in range(NEAR)
        ],
        axis=0,
    )


def nudge_kernel(all_ref, own_ref, obs_ref, relax_ref, high_ref, low_ref, sent_ref):
    base = GROUP * (lax.axis_index("near") % 2)
    level = base + lax.broadcasted_iota(jnp.int32, (PART, LEVELS), 0) // GROUP
    here = level == lax.broadcasted_iota(jnp.int32, (PART, LEVELS), 1)
    obs = jnp.sum(jnp.where(here, obs_ref[...], 0.0), axis=1, keepdims=True)
    relax = jnp.sum(jnp.where(here, relax_ref[...], 0.0), axis=1, keepdims=True)
    members = [slice(PART * k, PART * (k + 1)) for k in range(NEAR)]
    driver = all_ref[0, members[0], :]
    departures = [all_ref[f, m, :] - driver for f in range(FAR) for m in members]
    mean = sum(departures[1:], departures[0]) * (1.0 / MEMBERS)
    squares = [(d - mean) * (d - mean) for d in departures]
    spread = sum(squares[1:], squares[0]) * (1.0 / MEMBERS)
    gain = relax * spread / (spread + obs)
    misfit = jnp.concatenate([-gain * (own_ref[m, :] - driver) for m in members], axis=0)
    high, low = parts(swap_rows(misfit))
    count = NEAR * PART
    both = dot(jnp.concatenate([high, low], axis=0), high_ref[...], ((1,), (0,)))
    back = both[:count] + both[count:] + dot(high, low_ref[...], ((1,), (0,)))
    back = low_slots(back, 1)
    stacked = jnp.concatenate(
        [spread[:, TILES * k : TILES * (k + 1)] for k in range(OWN)], axis=0
    ).T
    first = stacked.astype(BF16).astype(F32)
    second = stacked - first
    for t in range(TILES):
        cols = slice(SLOTS * t, SLOTS * (t + 1))
        rows = jnp.concatenate([back[PART * l : PART * (l + 1), cols] for l in range(GROUP)], axis=1)
        extra = jnp.concatenate([first[t : t + 1], second[t : t + 1]], axis=0)
        pieces = []
        for k in range(NEAR):
            pieces += [rows[GROUP * k : GROUP * (k + 1)], extra]
        sent_ref[NEAR * CHUNK * t : NEAR * CHUNK * (t + 1), :] = jnp.concatenate(
            pieces, axis=0
        ).astype(BF16)


def apply_kernel(
    states_ref, got_ref, by_ref, wide_ref, out_ref, spread_ref, back, filled, mixed, turned, variance, sems
):
    def copy(c, h):
        part = (pl.ds(GROUP * c, GROUP), slice(None), pl.ds(HALF * h, HALF))
        return pltpu.make_async_copy(filled.at[part], out_ref.at[part], sems.at[2 * c + h])

    for t in range(TILES):
        rows = got_ref[NEAR * CHUNK * t : NEAR * CHUNK * (t + 1), :].astype(F32)
        for k in range(NEAR):
            row = SIDE * (k % 2) + 2 * t + k // 2
            extra = rows[CHUNK * k + GROUP : CHUNK * (k + 1)]
            mixed[row : row + 1, :] = extra[:1] + extra[1:]
    turned[...] = mixed[...].T
    for l in range(GROUP):
        strips = [turned[pl.ds(GROUP * l + k, OWN, stride=PART), :] for k in range(GROUP)]
        for c in range(2):
            variance[GROUP * c + l] = jnp.concatenate(
                [s[:, SIDE * c : SIDE * (c + 1)] for s in strips], axis=1
            )
    last = pltpu.make_async_copy(variance, spread_ref, sems.at[4])
    last.start()
    sign = signs(SIDE, GROUP).astype(BF16)
    count = GROUP * ROWS
    for c in range(2):
        for t in range(TILES):
            rows = got_ref[NEAR * CHUNK * t : NEAR * CHUNK * (t + 1), :].astype(F32)
            for k in range(2):
                r, row = 2 * t + k, CHUNK * (2 * k + c)
                back[c, GROUP * r : GROUP * (r + 1), :] = rows[row : row + GROUP]
        both = dot(wide_ref[...], back[c].astype(BF16).T, ((1,), (0,)))
        modes = (both[:count] + both[count:]).astype(BF16)
        for h in range(2):
            cols = slice(HALF * h, HALF * (h + 1))
            increment = dot(modes if h == 0 else modes * sign, by_ref[...], ((1,), (0,)))
            field = states_ref[GROUP * c : GROUP * (c + 1), :, cols].astype(F32)
            total = field + increment.reshape(GROUP, ROWS, HALF)
            filled[GROUP * c : GROUP * (c + 1), :, cols] = total.astype(BF16)
            copy(c, h).start()
    for c in range(2):
        for h in range(2):
            copy(c, h).wait()
    last.wait()


def call(kernel, outs, limit=24 * MIB, **kw):
    return pl.pallas_call(
        kernel,
        out_shape=outs,
        compiler_params=pltpu.CompilerParams(vmem_limit_bytes=limit),
        **kw,
    )


def shape(dims, dtype):
    return jax.ShapeDtypeStruct(dims, dtype)


def per_device(consts, states, obs_var, relax_rate):
    bx_high, bx_low, bx_high_t, bx_low_t, by, by_t, narrow, widen = consts
    field = states[0]
    hbm = pl.BlockSpec(memory_space=pltpu.HBM)
    vmem = pl.BlockSpec(memory_space=pltpu.VMEM)
    devices, lanes, columns = TILES * NEAR, GROUP * SLOTS, NEAR * PART

    def exchange(rows):
        chunks = rows.reshape(devices, rows.shape[0] // (2 * devices), 2, lanes)
        return lax.all_to_all(chunks, ("tile", "near"), 0, 0, tiled=True).reshape(rows.shape)

    sent = call(
        project_kernel,
        shape((devices * GROUP, lanes), BF16),
        in_specs=[hbm] * 3,
        out_specs=vmem,
        scratch_shapes=[
            pltpu.VMEM((STEPS, 2, LEVELS, ROWS, WIDTH), BF16),
            pltpu.VMEM((STEPS, WIDTH, MODES), BF16),
            pltpu.VMEM((2 * lanes, GROUP * ROWS), BF16),
            pltpu.VMEM((2 * LEVELS * ROWS, MODES), F32),
            pltpu.SemaphoreType.DMA((3 * STEPS + 1,)),
        ],
    )(*(pltpu.with_memory_space_constraint(x, pltpu.HBM) for x in (field, by, narrow)))
    coeffs, copies = call(
        coeffs_kernel,
        (shape((columns, MODES), F32), shape((FAR, columns, MODES), F32)),
        in_specs=[vmem] * 3,
        out_specs=(vmem, vmem),
        scratch_shapes=[pltpu.VMEM((columns, TILES * SLOTS), BF16)],
    )(exchange(sent), bx_high, bx_low)
    gathered = lax.all_to_all(copies, "far", 0, 0, tiled=True)
    sent = call(
        nudge_kernel,
        shape((devices * CHUNK, lanes), BF16),
        in_specs=[vmem] * 6,
        out_specs=vmem,
    )(gathered, coeffs, obs_var[None], relax_rate[None], bx_high_t, bx_low_t)
    nudged, spread = call(
        apply_kernel,
        (shape((LEVELS, ROWS, N), BF16), shape((LEVELS, OWN, MODES), F32)),
        in_specs=[vmem] * 4,
        out_specs=(hbm, hbm),
        scratch_shapes=[
            pltpu.VMEM((2, MODES, lanes), F32),
            pltpu.VMEM((LEVELS, ROWS, N), BF16),
            pltpu.VMEM((2 * SIDE, lanes), F32),
            pltpu.VMEM((lanes, 2 * SIDE), F32),
            pltpu.VMEM((LEVELS, OWN, MODES), F32),
            pltpu.SemaphoreType.DMA((5,)),
        ],
    )(field, exchange(sent), by_t, widen)
    return nudged[None], spread


def solution(mesh):
    fine = Mesh(mesh.devices.reshape(FAR, NEAR, TILES), ("far", "near", "tile"))
    rows = P(("far", "near"), None, "tile", None)
    return jax.shard_map(
        functools.partial(per_device, tables()),
        mesh=fine,
        in_specs=(rows, P(), P()),
        out_specs=(rows, P(None, "tile", None)),
        check_vma=False,
    )
```

```python
import functools
import math

import jax
import jax.numpy as jnp
import numpy as np
from jax import lax
from jax.experimental import pallas as pl
from jax.experimental.pallas import tpu as pltpu
from jax.sharding import Mesh, PartitionSpec as P

N = 2048
MODES = 256
LEVELS = 8
MEMBERS = 16
TILES = 32
ROWS = N // TILES
NEAR = 4
FAR = MEMBERS // NEAR
OWN = MODES // TILES
STEPS = 4
HALF = N // 2
WIDTH = HALF // STEPS
SLOTS = 32
RANK = 20
GROUP = 4
SIDE = MODES // GROUP
KEPT = SLOTS - OWN
PART = NEAR * GROUP
MIB = 1024 * 1024
BF16 = jnp.bfloat16
F32 = jnp.float32


def mode_table():
    mode = np.arange(MODES)[None, :]
    phases = (np.arange(N)[:, None] * ((mode + 1) // 2)) % N
    angles = 2.0 * math.pi / N * phases
    scaled = np.where(mode % 2 == 1, np.sin(angles), np.cos(angles))
    factor = np.where(mode == 0, math.sqrt(1.0 / N), math.sqrt(2.0 / N))
    return scaled * factor


def row_basis():
    n = np.arange(ROWS)
    centre = ((ROWS - 1 - 2 * n) / 2.0) ** 2 * math.cos(math.pi * MODES / N)
    beside = n[1:] * (ROWS - n[1:]) / 2.0
    vectors = np.linalg.eigh(np.diag(centre) + np.diag(beside, 1) + np.diag(beside, -1))[1]
    basis = vectors[:, ::-1][:, :RANK]
    return basis * np.sign(basis[0])


def split(table):
    high = table.astype(np.float32).astype(BF16)
    return high, (table - high.astype(np.float64)).astype(np.float32).astype(BF16)


def tables():
    full = mode_table()
    flip = lambda a: np.ascontiguousarray(a.T)
    first = np.arange(MODES).reshape(TILES, OWN).T.reshape(-1)
    second = np.arange(MODES).reshape(GROUP, SIDE).T.reshape(-1)
    slots = np.concatenate([np.arange(RANK), np.arange(SLOTS - RANK)])
    basis = row_basis()
    blocks = full.reshape(TILES, ROWS, MODES)
    modes = np.stack(
        [(blocks * basis[:, k][None, :, None]).sum(axis=1) for k in range(RANK)], axis=1
    )
    bx_high, bx_low = split(modes[:, slots][:, :, first].reshape(TILES * SLOTS, MODES))
    kept = (np.arange(SLOTS) < KEPT).astype(np.float64)
    returned = (modes[:, slots] * kept[:, None])[:, :, first].reshape(TILES * SLOTS, MODES)
    back_high, back_low = split(flip(returned))
    narrow = np.kron(np.eye(GROUP), basis[:, slots].T)
    narrow_high, narrow_low = split(narrow)
    by = full[:HALF].astype(np.float32).astype(BF16)[:, second]
    narrow_both = np.concatenate([narrow_high, narrow_low], axis=0)
    wide = split(np.kron(np.eye(GROUP), basis[:, slots] * kept))
    return bx_high, bx_low, back_high, back_low, by, flip(by), narrow_both, np.concatenate(wide)


def signs(major, minor):
    column = lax.broadcasted_iota(jnp.int32, (1, MODES), 1)
    mode = major * (column % minor) + column // minor
    return (1 - 2 * ((mode + 1) // 2 % 2)).astype(F32)


def dot(a, b, dims):
    return lax.dot_general(a, b, (dims, ((), ())), preferred_element_type=F32)


def parts(values):
    high = values.astype(BF16)
    return high, (values - high.astype(F32)).astype(BF16)


def low_slots(values, axis):
    slot = lax.broadcasted_iota(jnp.int32, values.shape, axis) % SLOTS
    rounded = values.astype(BF16).astype(F32)
    return jnp.where(slot < RANK, rounded, values - rounded)


def project_kernel(states_ref, by_ref, narrow_ref, out_ref, field, table, small, acc, sems):
    last = pltpu.make_async_copy(narrow_ref, small, sems.at[3 * STEPS])

    def copies(k):
        rows = pl.ds(WIDTH * k, WIDTH)
        yield pltpu.make_async_copy(by_ref.at[rows, :], table.at[k], sems.at[3 * k])
        for h in range(2):
            cols = pl.ds(HALF * h + WIDTH * k, WIDTH)
            yield pltpu.make_async_copy(
                states_ref.at[:, :, cols], field.at[k, h], sems.at[3 * k + 1 + h]
            )

    for k in range(STEPS):
        for c in copies(k):
            c.start()
    last.start()
    for k in range(STEPS):
        for c in copies(k):
            c.wait()
        for h in range(2):
            part = dot(field[k, h].reshape(LEVELS * ROWS, WIDTH), table[k], ((1,), (0,)))
            rows = slice(LEVELS * ROWS * h, LEVELS * ROWS * (h + 1))
            acc[rows, :] = part if k == 0 else acc[rows, :] + part
    last.wait()
    sign = signs(SIDE, GROUP)
    count = GROUP * SLOTS
    sides = []
    for c in range(2):
        lower = acc[GROUP * ROWS * c : GROUP * ROWS * (c + 1), :]
        upper = acc[GROUP * ROWS * (c + 2) : GROUP * ROWS * (c + 3), :]
        high, low = parts(lower + sign * upper)
        both = dot(small[...], high, ((1,), (0,)))
        narrow = both[:count] + both[count:] + dot(small[:count, :], low, ((1,), (0,)))
        sides.append(low_slots(narrow, 0).T)
    for r in range(SIDE // 2):
        rows = []
        for k in range(2):
            for side in sides:
                rows.append(side[GROUP * (2 * r + k) : GROUP * (2 * r + k + 1)])
        out_ref[4 * GROUP * r : 4 * GROUP * (r + 1), :] = jnp.concatenate(rows, axis=0).astype(BF16)


def coeffs_kernel(rows_ref, high_ref, low_ref, out_ref, copies_ref, wide):
    lanes = GROUP * SLOTS
    for u in range(TILES // GROUP):
        pieces = [rows_ref[PART * (GROUP * u + k) : PART * (GROUP * u + k + 1), :] for k in range(GROUP)]
        for l in range(GROUP):
            wide[PART * l : PART * (l + 1), lanes * u : lanes * (u + 1)] = jnp.concatenate(
                [p[:, SLOTS * l : SLOTS * (l + 1)] for p in pieces], axis=1
            )
    x = wide[...]
    coeffs = dot(x, high_ref[...], ((1,), (0,))) + dot(x, low_ref[...], ((1,), (0,)))
    coeffs = swap_rows(coeffs)
    out_ref[...] = coeffs
    for k in range(FAR):
        copies_ref[k] = coeffs


def swap_rows(values):
    return jnp.concatenate(
        [
            values[PART * l + GROUP * k : PART * l + GROUP * (k + 1)]
            for k in range(GROUP)
            for l in range(NEAR)
        ],
        axis=0,
    )


def nudge_kernel(all_ref, own_ref, obs_ref, relax_ref, high_ref, low_ref, sent_ref):
    base = GROUP * (lax.axis_index("near") % 2)
    level = base + lax.broadcasted_iota(jnp.int32, (PART, LEVELS), 0) // GROUP
    here = level == lax.broadcasted_iota(jnp.int32, (PART, LEVELS), 1)
    obs = jnp.sum(jnp.where(here, obs_ref[...], 0.0), axis=1, keepdims=True)
    relax = jnp.sum(jnp.where(here, relax_ref[...], 0.0), axis=1, keepdims=True)
    members = [slice(PART * k, PART * (k + 1)) for k in range(NEAR)]
    driver = all_ref[0, members[0], :]
    departures = [all_ref[f, m, :] - driver for f in range(FAR) for m in members]
    mean = sum(departures[1:], departures[0]) * (1.0 / MEMBERS)
    squares = [(d - mean) * (d - mean) for d in departures]
    spread = sum(squares[1:], squares[0]) * (1.0 / MEMBERS)
    gain = relax * spread / (spread + obs)
    misfit = jnp.concatenate([-gain * (own_ref[m, :] - driver) for m in members], axis=0)
    high, low = parts(swap_rows(misfit))
    count = NEAR * PART
    both = dot(jnp.concatenate([high, low], axis=0), high_ref[...], ((1,), (0,)))
    back = both[:count] + both[count:] + dot(high, low_ref[...], ((1,), (0,)))
    row = lax.broadcasted_iota(jnp.int32, (MODES, TILES * SLOTS), 0)
    lane = lax.broadcasted_iota(jnp.int32, (MODES, TILES * SLOTS), 1)
    target = TILES * (lane % SLOTS - KEPT) + lane // SLOTS
    place = jnp.where(row == target, 1.0, 0.0).astype(BF16)
    spreads = swap_rows(jnp.concatenate([spread] * NEAR, axis=0)).astype(BF16)
    back = (low_slots(back, 1) + dot(spreads, place, ((1,), (0,)))).astype(BF16)
    for t in range(TILES):
        cols = slice(SLOTS * t, SLOTS * (t + 1))
        sent_ref[PART * t : PART * (t + 1), :] = jnp.concatenate(
            [back[PART * l : PART * (l + 1), cols] for l in range(GROUP)], axis=1
        )


def apply_kernel(
    states_ref, got_ref, by_ref, wide_ref, out_ref, spread_ref, back, filled, variance, sems
):
    def copy(c, h):
        part = (pl.ds(GROUP * c, GROUP), slice(None), pl.ds(HALF * h, HALF))
        return pltpu.make_async_copy(filled.at[part], out_ref.at[part], sems.at[2 * c + h])

    sign = signs(SIDE, GROUP).astype(BF16)
    count = GROUP * ROWS
    row = lax.broadcasted_iota(jnp.int32, (MODES, MODES), 0)
    lane = lax.broadcasted_iota(jnp.int32, (MODES, MODES), 1)
    order = jnp.where(lane == SIDE * (row % GROUP) + row // GROUP, 1.0, 0.0).astype(BF16)
    for c in range(2):
        for r in range(SIDE // 2):
            rows = got_ref[4 * GROUP * r : 4 * GROUP * (r + 1), :].astype(F32)
            for k in range(2):
                start = GROUP * (2 * k + c)
                to = GROUP * (2 * r + k)
                back[to : to + GROUP, :] = rows[start : start + GROUP]
        slots = back[...].T
        spreads = jnp.concatenate(
            [slots[SLOTS * l + KEPT : SLOTS * (l + 1)] for l in range(GROUP)], axis=0
        ).astype(BF16)
        variance[GROUP * c : GROUP * (c + 1)] = dot(spreads, order, ((1,), (0,))).reshape(
            GROUP, OWN, MODES
        )
        both = dot(wide_ref[...], slots.astype(BF16), ((1,), (0,)))
        modes = (both[:count] + both[count:]).astype(BF16)
        for h in range(2):
            cols = slice(HALF * h, HALF * (h + 1))
            increment = dot(modes if h == 0 else modes * sign, by_ref[...], ((1,), (0,)))
            field = states_ref[GROUP * c : GROUP * (c + 1), :, cols].astype(F32)
            total = field + increment.reshape(GROUP, ROWS, HALF)
            if c == 1 and h == 0:
                last = pltpu.make_async_copy(variance, spread_ref, sems.at[4])
                last.start()
            filled[GROUP * c : GROUP * (c + 1), :, cols] = total.astype(BF16)
            copy(c, h).start()
    for c in range(2):
        for h in range(2):
            copy(c, h).wait()
    last.wait()


def call(kernel, outs, limit=24 * MIB, **kw):
    return pl.pallas_call(
        kernel,
        out_shape=outs,
        compiler_params=pltpu.CompilerParams(vmem_limit_bytes=limit),
        **kw,
    )


def shape(dims, dtype):
    return jax.ShapeDtypeStruct(dims, dtype)


def per_device(consts, states, obs_var, relax_rate):
    bx_high, bx_low, back_high, back_low, by, by_t, narrow, widen = consts
    field = states[0]
    hbm = pl.BlockSpec(memory_space=pltpu.HBM)
    vmem = pl.BlockSpec(memory_space=pltpu.VMEM)
    devices, lanes, columns = TILES * NEAR, GROUP * SLOTS, NEAR * PART

    def exchange(rows):
        chunks = rows.reshape(devices, rows.shape[0] // (2 * devices), 2, lanes)
        return lax.all_to_all(chunks, ("tile", "near"), 0, 0, tiled=True).reshape(rows.shape)

    sent = call(
        project_kernel,
        shape((devices * GROUP, lanes), BF16),
        in_specs=[hbm] * 3,
        out_specs=vmem,
        scratch_shapes=[
            pltpu.VMEM((STEPS, 2, LEVELS, ROWS, WIDTH), BF16),
            pltpu.VMEM((STEPS, WIDTH, MODES), BF16),
            pltpu.VMEM((2 * lanes, GROUP * ROWS), BF16),
            pltpu.VMEM((2 * LEVELS * ROWS, MODES), F32),
            pltpu.SemaphoreType.DMA((3 * STEPS + 1,)),
        ],
    )(*(pltpu.with_memory_space_constraint(x, pltpu.HBM) for x in (field, by, narrow)))
    coeffs, copies = call(
        coeffs_kernel,
        (shape((columns, MODES), F32), shape((FAR, columns, MODES), F32)),
        in_specs=[vmem] * 3,
        out_specs=(vmem, vmem),
        scratch_shapes=[pltpu.VMEM((columns, TILES * SLOTS), BF16)],
    )(exchange(sent), bx_high, bx_low)
    gathered = lax.all_to_all(copies, "far", 0, 0, tiled=True)
    sent = call(
        nudge_kernel,
        shape((devices * GROUP, lanes), BF16),
        in_specs=[vmem] * 6,
        out_specs=vmem,
    )(gathered, coeffs, obs_var[None], relax_rate[None], back_high, back_low)
    nudged, spread = call(
        apply_kernel,
        (shape((LEVELS, ROWS, N), BF16), shape((LEVELS, OWN, MODES), F32)),
        in_specs=[vmem] * 4,
        out_specs=(hbm, hbm),
        scratch_shapes=[
            pltpu.VMEM((MODES, lanes), F32),
            pltpu.VMEM((LEVELS, ROWS, N), BF16),
            pltpu.VMEM((LEVELS, OWN, MODES), F32),
            pltpu.SemaphoreType.DMA((5,)),
        ],
    )(field, exchange(sent), by_t, widen)
    return nudged[None], spread


def solution(mesh):
    fine = Mesh(mesh.devices.reshape(FAR, NEAR, TILES), ("far", "near", "tile"))
    rows = P(("far", "near"), None, "tile", None)
    return jax.shard_map(
        functools.partial(per_device, tables()),
        mesh=fine,
        in_specs=(rows, P(), P()),
        out_specs=(rows, P(None, "tile", None)),
        check_vma=False,
    )
```

```python
import functools
import math

import jax
import jax.numpy as jnp
import numpy as np
from jax import lax
from jax.experimental import pallas as pl
from jax.experimental.pallas import tpu as pltpu
from jax.sharding import Mesh, PartitionSpec as P

N = 2048
MODES = 256
LEVELS = 8
MEMBERS = 16
TILES = 32
ROWS = N // TILES
NEAR = 4
FAR = MEMBERS // NEAR
OWN = MODES // TILES
STEPS = 4
HALF = N // 2
WIDTH = HALF // STEPS
SLOTS = 32
RANK = 20
GROUP = 4
SIDE = MODES // GROUP
KEPT = SLOTS - OWN
PART = NEAR * GROUP
MIB = 1024 * 1024
BF16 = jnp.bfloat16
F32 = jnp.float32


def mode_table():
    mode = np.arange(MODES)[None, :]
    phases = (np.arange(N)[:, None] * ((mode + 1) // 2)) % N
    angles = 2.0 * math.pi / N * phases
    scaled = np.where(mode % 2 == 1, np.sin(angles), np.cos(angles))
    factor = np.where(mode == 0, math.sqrt(1.0 / N), math.sqrt(2.0 / N))
    return scaled * factor


def row_basis():
    n = np.arange(ROWS)
    centre = ((ROWS - 1 - 2 * n) / 2.0) ** 2 * math.cos(math.pi * MODES / N)
    beside = n[1:] * (ROWS - n[1:]) / 2.0
    vectors = np.linalg.eigh(np.diag(centre) + np.diag(beside, 1) + np.diag(beside, -1))[1]
    basis = vectors[:, ::-1][:, :RANK]
    return basis * np.sign(basis[0])


def split(table):
    high = table.astype(np.float32).astype(BF16)
    return high, (table - high.astype(np.float64)).astype(np.float32).astype(BF16)


def tables():
    full = mode_table()
    flip = lambda a: np.ascontiguousarray(a.T)
    first = np.arange(MODES).reshape(TILES, OWN).T.reshape(-1)
    second = np.arange(MODES).reshape(GROUP, SIDE).T.reshape(-1)
    slots = np.concatenate([np.arange(RANK), np.arange(SLOTS - RANK)])
    basis = row_basis()
    blocks = full.reshape(TILES, ROWS, MODES)
    modes = np.stack(
        [(blocks * basis[:, k][None, :, None]).sum(axis=1) for k in range(RANK)], axis=1
    )
    bx_high, bx_low = split(modes[:, slots][:, :, first].reshape(TILES * SLOTS, MODES))
    kept = (np.arange(SLOTS) < KEPT).astype(np.float64)
    narrow = np.kron(np.eye(GROUP), basis[:, slots].T)
    narrow_high, narrow_low = split(narrow)
    by = full[:HALF].astype(np.float32).astype(BF16)[:, second]
    narrow_both = np.concatenate([narrow_high, narrow_low], axis=0)
    wide = split(np.kron(np.eye(GROUP), basis[:, slots] * kept))
    return bx_high, bx_low, by, flip(by), narrow_both, np.concatenate(wide)


def signs(major, minor):
    column = lax.broadcasted_iota(jnp.int32, (1, MODES), 1)
    mode = major * (column % minor) + column // minor
    return (1 - 2 * ((mode + 1) // 2 % 2)).astype(F32)


def dot(a, b, dims):
    return lax.dot_general(a, b, (dims, ((), ())), preferred_element_type=F32)


def parts(values):
    high = values.astype(BF16)
    return high, (values - high.astype(F32)).astype(BF16)


def low_slots(values, axis):
    slot = lax.broadcasted_iota(jnp.int32, values.shape, axis) % SLOTS
    rounded = values.astype(BF16).astype(F32)
    return jnp.where(slot < RANK, rounded, values - rounded)


def project_kernel(states_ref, by_ref, narrow_ref, out_ref, field, table, small, acc, sems):
    last = pltpu.make_async_copy(narrow_ref, small, sems.at[3 * STEPS])

    def copies(k):
        rows = pl.ds(WIDTH * k, WIDTH)
        yield pltpu.make_async_copy(by_ref.at[rows, :], table.at[k], sems.at[3 * k])
        for h in range(2):
            cols = pl.ds(HALF * h + WIDTH * k, WIDTH)
            yield pltpu.make_async_copy(
                states_ref.at[:, :, cols], field.at[k, h], sems.at[3 * k + 1 + h]
            )

    for k in range(STEPS):
        for c in copies(k):
            c.start()
    last.start()
    for k in range(STEPS):
        for c in copies(k):
            c.wait()
        for h in range(2):
            part = dot(field[k, h].reshape(LEVELS * ROWS, WIDTH), table[k], ((1,), (0,)))
            rows = slice(LEVELS * ROWS * h, LEVELS * ROWS * (h + 1))
            acc[rows, :] = part if k == 0 else acc[rows, :] + part
    last.wait()
    sign = signs(SIDE, GROUP)
    count = GROUP * SLOTS
    sides = []
    for c in range(2):
        lower = acc[GROUP * ROWS * c : GROUP * ROWS * (c + 1), :]
        upper = acc[GROUP * ROWS * (c + 2) : GROUP * ROWS * (c + 3), :]
        high, low = parts(lower + sign * upper)
        both = dot(small[...], high, ((1,), (0,)))
        narrow = both[:count] + both[count:] + dot(small[:count, :], low, ((1,), (0,)))
        sides.append(low_slots(narrow, 0).T)
    for r in range(SIDE // 2):
        rows = []
        for k in range(2):
            for side in sides:
                rows.append(side[GROUP * (2 * r + k) : GROUP * (2 * r + k + 1)])
        out_ref[4 * GROUP * r : 4 * GROUP * (r + 1), :] = jnp.concatenate(rows, axis=0).astype(BF16)


def coeffs_kernel(rows_ref, high_ref, low_ref, out_ref, copies_ref, wide):
    lanes = GROUP * SLOTS
    for u in range(TILES // GROUP):
        pieces = [rows_ref[PART * (GROUP * u + k) : PART * (GROUP * u + k + 1), :] for k in range(GROUP)]
        for l in range(GROUP):
            wide[PART * l : PART * (l + 1), lanes * u : lanes * (u + 1)] = jnp.concatenate(
                [p[:, SLOTS * l : SLOTS * (l + 1)] for p in pieces], axis=1
            )
    x = wide[...]
    coeffs = dot(x, high_ref[...], ((1,), (0,))) + dot(x, low_ref[...], ((1,), (0,)))
    coeffs = swap_rows(coeffs)
    out_ref[...] = coeffs
    for k in range(FAR):
        copies_ref[k] = coeffs


def swap_rows(values):
    return jnp.concatenate(
        [
            values[PART * l + GROUP * k : PART * l + GROUP * (k + 1)]
            for k in range(GROUP)
            for l in range(NEAR)
        ],
        axis=0,
    )


def nudge_kernel(all_ref, own_ref, obs_ref, relax_ref, high_ref, low_ref, sent_ref):
    base = GROUP * (lax.axis_index("near") % 2)
    level = base + lax.broadcasted_iota(jnp.int32, (PART, LEVELS), 0) // GROUP
    here = level == lax.broadcasted_iota(jnp.int32, (PART, LEVELS), 1)
    obs = jnp.sum(jnp.where(here, obs_ref[...], 0.0), axis=1, keepdims=True)
    relax = jnp.sum(jnp.where(here, relax_ref[...], 0.0), axis=1, keepdims=True)
    members = [slice(PART * k, PART * (k + 1)) for k in range(NEAR)]
    driver = all_ref[0, members[0], :]
    departures = [all_ref[f, m, :] - driver for f in range(FAR) for m in members]
    mean = sum(departures[1:], departures[0]) * (1.0 / MEMBERS)
    squares = [(d - mean) * (d - mean) for d in departures]
    spread = sum(squares[1:], squares[0]) * (1.0 / MEMBERS)
    gain = relax * spread / (spread + obs)
    misfit = jnp.concatenate([-gain * (own_ref[m, :] - driver) for m in members], axis=0)
    high, low = parts(swap_rows(misfit))
    count = NEAR * PART
    both = dot(jnp.concatenate([high, low], axis=0), high_ref[...], ((1,), (1,)))
    back = both[:count] + both[count:] + dot(high, low_ref[...], ((1,), (1,)))
    row = lax.broadcasted_iota(jnp.int32, (MODES, TILES * SLOTS), 0)
    lane = lax.broadcasted_iota(jnp.int32, (MODES, TILES * SLOTS), 1)
    target = TILES * (lane % SLOTS - KEPT) + lane // SLOTS
    place = jnp.where(row == target, 1.0, 0.0).astype(BF16)
    spreads = swap_rows(jnp.concatenate([spread] * NEAR, axis=0)).astype(BF16)
    slot = lax.broadcasted_iota(jnp.int32, back.shape, 1) % SLOTS
    placed = dot(spreads, place, ((1,), (0,)))
    back = jnp.where(slot < KEPT, low_slots(back, 1), placed).astype(BF16)
    for t in range(TILES):
        cols = slice(SLOTS * t, SLOTS * (t + 1))
        sent_ref[PART * t : PART * (t + 1), :] = jnp.concatenate(
            [back[PART * l : PART * (l + 1), cols] for l in range(GROUP)], axis=1
        )


def apply_kernel(
    states_ref, got_ref, by_ref, wide_ref, out_ref, spread_ref, back, filled, variance, sems
):
    def copy(c, h):
        part = (pl.ds(GROUP * c, GROUP), slice(None), pl.ds(HALF * h, HALF))
        return pltpu.make_async_copy(filled.at[part], out_ref.at[part], sems.at[2 * c + h])

    sign = signs(SIDE, GROUP).astype(BF16)
    count = GROUP * ROWS
    row = lax.broadcasted_iota(jnp.int32, (MODES, MODES), 0)
    lane = lax.broadcasted_iota(jnp.int32, (MODES, MODES), 1)
    order = jnp.where(lane == SIDE * (row % GROUP) + row // GROUP, 1.0, 0.0).astype(BF16)
    for c in range(2):
        for r in range(SIDE // 2):
            rows = got_ref[4 * GROUP * r : 4 * GROUP * (r + 1), :].astype(F32)
            for k in range(2):
                start = GROUP * (2 * k + c)
                to = GROUP * (2 * r + k)
                back[to : to + GROUP, :] = rows[start : start + GROUP]
        slots = back[...].T
        spreads = jnp.concatenate(
            [slots[SLOTS * l + KEPT : SLOTS * (l + 1)] for l in range(GROUP)], axis=0
        ).astype(BF16)
        variance[GROUP * c : GROUP * (c + 1)] = dot(spreads, order, ((1,), (0,))).reshape(
            GROUP, OWN, MODES
        )
        both = dot(wide_ref[...], slots.astype(BF16), ((1,), (0,)))
        modes = (both[:count] + both[count:]).astype(BF16)
        for h in range(2):
            cols = slice(HALF * h, HALF * (h + 1))
            increment = dot(modes if h == 0 else modes * sign, by_ref[...], ((1,), (0,)))
            field = states_ref[GROUP * c : GROUP * (c + 1), :, cols].astype(F32)
            total = field + increment.reshape(GROUP, ROWS, HALF)
            if c == 1 and h == 0:
                last = pltpu.make_async_copy(variance, spread_ref, sems.at[4])
                last.start()
            filled[GROUP * c : GROUP * (c + 1), :, cols] = total.astype(BF16)
            copy(c, h).start()
    for c in range(2):
        for h in range(2):
            copy(c, h).wait()
    last.wait()


def call(kernel, outs, limit=24 * MIB, **kw):
    return pl.pallas_call(
        kernel,
        out_shape=outs,
        compiler_params=pltpu.CompilerParams(vmem_limit_bytes=limit),
        **kw,
    )


def shape(dims, dtype):
    return jax.ShapeDtypeStruct(dims, dtype)


def per_device(consts, states, obs_var, relax_rate):
    bx_high, bx_low, by, by_t, narrow, widen = consts
    field = states[0]
    hbm = pl.BlockSpec(memory_space=pltpu.HBM)
    vmem = pl.BlockSpec(memory_space=pltpu.VMEM)
    devices, lanes, columns = TILES * NEAR, GROUP * SLOTS, NEAR * PART

    def exchange(rows):
        chunks = rows.reshape(devices, rows.shape[0] // (2 * devices), 2, lanes)
        return lax.all_to_all(chunks, ("tile", "near"), 0, 0, tiled=True).reshape(rows.shape)

    sent = call(
        project_kernel,
        shape((devices * GROUP, lanes), BF16),
        in_specs=[hbm] * 3,
        out_specs=vmem,
        scratch_shapes=[
            pltpu.VMEM((STEPS, 2, LEVELS, ROWS, WIDTH), BF16),
            pltpu.VMEM((STEPS, WIDTH, MODES), BF16),
            pltpu.VMEM((2 * lanes, GROUP * ROWS), BF16),
            pltpu.VMEM((2 * LEVELS * ROWS, MODES), F32),
            pltpu.SemaphoreType.DMA((3 * STEPS + 1,)),
        ],
    )(*(pltpu.with_memory_space_constraint(x, pltpu.HBM) for x in (field, by, narrow)))
    coeffs, copies = call(
        coeffs_kernel,
        (shape((columns, MODES), F32), shape((FAR, columns, MODES), F32)),
        in_specs=[vmem] * 3,
        out_specs=(vmem, vmem),
        scratch_shapes=[pltpu.VMEM((columns, TILES * SLOTS), BF16)],
    )(exchange(sent), bx_high, bx_low)
    gathered = lax.all_to_all(copies, "far", 0, 0, tiled=True)
    sent = call(
        nudge_kernel,
        shape((devices * GROUP, lanes), BF16),
        in_specs=[vmem] * 6,
        out_specs=vmem,
    )(gathered, coeffs, obs_var[None], relax_rate[None], bx_high, bx_low)
    nudged, spread = call(
        apply_kernel,
        (shape((LEVELS, ROWS, N), BF16), shape((LEVELS, OWN, MODES), F32)),
        in_specs=[vmem] * 4,
        out_specs=(hbm, hbm),
        scratch_shapes=[
            pltpu.VMEM((MODES, lanes), F32),
            pltpu.VMEM((LEVELS, ROWS, N), BF16),
            pltpu.VMEM((LEVELS, OWN, MODES), F32),
            pltpu.SemaphoreType.DMA((5,)),
        ],
    )(field, exchange(sent), by_t, widen)
    return nudged[None], spread


def solution(mesh):
    fine = Mesh(mesh.devices.reshape(FAR, NEAR, TILES), ("far", "near", "tile"))
    rows = P(("far", "near"), None, "tile", None)
    return jax.shard_map(
        functools.partial(per_device, tables()),
        mesh=fine,
        in_specs=(rows, P(), P()),
        out_specs=(rows, P(None, "tile", None)),
        check_vma=False,
    )
```
